32 devices in a mesh: seq: 8 (over z, y), head: 4 (over x, core).
Axes of the slice: x: 2, y: 2, z: 4, core: 2. Of those that a mesh axis runs over, the one named last changes fastest.
Arguments:
- query_rows: bfloat16 [16384, 4096], P(('seq', 'head')), may hold values from -200 to 200
- key_rows: bfloat16 [16384, 512], P(('seq', 'head')), may hold values from -18 to 18
- value_rows: bfloat16 [16384, 512], P(('seq', 'head')), may hold values from -6 to 6
- random_table: int32 [128, 4, 3], replicated, may hold values from 0 to 127, as said below
- global_blocks: int32 [2], replicated, may hold values from 0 to 127
Outputs:
- attended: bfloat16 [16384, 4096], P(('seq', 'head'))
The draws below stay inside these ranges and needn't reach their ends.
Inputs may be any that keep to these rules, and one draw needn't show every extreme that they name: `random_table`: for each of the 4 head groups and each aligned run of 16 query blocks (those of one index of seq), with the owner of block j being j // 16: at most 6 of the run's 3 * 16 entries name blocks of one owner, and they name at most 3 distinct blocks of one owner; both bounds are reached.
All inputs are finite; a program needn't handle non-finite values.
Results may differ from the reference program's by a relative error of at most 0.0029.
Values may be sent and summed in bfloat16 or wider, within the bound.
No kernel may reach another device: no remote copies, remote signals or barrier semaphores. Data moves between devices by JAX's collectives and lax.ppermute only.
A program may use at most 128 MiB of HBM per device.

```python
import math
import jax
import jax.numpy as jnp
from jax import lax

BLOCK = 128
HEAD_DIM = 128
Q_HEADS = 32
KV_HEADS = 4
GLOBALS = 2
RANDOM = 3
BLK_DEV = 16
BLOCKS = 128
TOKENS = 16384
CAP_RAW = 6
DISTINCT = 3


def pair_rows(key):
    normal_keys = jax.random.normal(jax.random.fold_in(key, 701), (TOKENS, KV_HEADS * HEAD_DIM), jnp.float32)
    key_part = jnp.clip(3.0 * normal_keys, -18.0, 18.0)
    queries = jnp.clip(jax.random.normal(jax.random.fold_in(key, 702), (TOKENS, Q_HEADS * HEAD_DIM), jnp.float32), -6.0, 6.0)
    return (queries, key_part)


def draw_query_rows(key, part):
    return pair_rows(key)[0].astype(jnp.bfloat16)


def draw_key_rows(key, part):
    return pair_rows(key)[1].astype(jnp.bfloat16)


def draw_random_table(key, part):
    entry_count = RANDOM * BLK_DEV
    seq_count = BLOCKS // BLK_DEV
    group_count = (entry_count + CAP_RAW - 1) // CAP_RAW

    def one_run(run_key):
        owners = jax.random.permutation(jax.random.fold_in(run_key, 1), seq_count)
        groups = jnp.arange(entry_count, dtype=jnp.int32) // CAP_RAW
        pair_index = jnp.arange(entry_count, dtype=jnp.int32) % CAP_RAW // 2
        group_keys = jax.vmap(lambda which: jax.random.fold_in(run_key, 50 + which))(jnp.arange(group_count, dtype=jnp.int32))
        picks = jax.vmap(lambda gkey: jax.random.permutation(gkey, BLK_DEV)[:DISTINCT])(group_keys)
        local_ids = picks[groups, pair_index]
        references = owners[groups] * BLK_DEV + local_ids
        shuffle = jax.random.permutation(jax.random.fold_in(run_key, 5), entry_count)
        return references[shuffle].reshape(BLK_DEV, RANDOM)
    run_keys = jax.vmap(lambda which: jax.random.fold_in(key, 900 + which))(jnp.arange(seq_count * KV_HEADS, dtype=jnp.int32))
    tables = jax.vmap(one_run)(run_keys).reshape(seq_count, KV_HEADS, BLK_DEV, RANDOM)
    return tables.transpose(0, 2, 1, 3).reshape(BLOCKS, KV_HEADS, RANDOM).astype(jnp.int32)


def level_of(own_key, extent, pieces, low, top_value):
    factor_of = 1.0
    for position, shards_of in pieces:
        heights = jax.random.uniform(jax.random.fold_in(jax.random.fold_in(own_key, 6), position), (shards_of,), jnp.float32, low / len(pieces), top_value / len(pieces))
        factor_of = factor_of * jnp.repeat(jnp.exp(heights), extent[position] // shards_of).reshape((-1,) + (1,) * (len(extent) - 1 - position))
    return factor_of


def noise(stream_key, shape, deviation, most, shards=(), kind=jnp.bfloat16):
    drawn = deviation * jax.random.normal(stream_key, shape, jnp.float32)
    if shards:
        drawn = drawn * level_of(stream_key, shape, shards, -0.22, 0.18)
    return jnp.clip(drawn, -most, most).astype(kind)


def setup_inputs(seed: int = 0) -> dict:
    arg_keys = jax.random.split(jax.random.key(seed), 6)
    return {
        "query_rows": draw_query_rows(jax.random.fold_in(arg_keys[5], 71), 0),
        "key_rows": draw_key_rows(jax.random.fold_in(arg_keys[5], 71), 0),
        "value_rows": noise(arg_keys[2], (TOKENS, KV_HEADS * HEAD_DIM), 1.0, 6.0, ((0, 32),)),
        "random_table": draw_random_table(jax.random.fold_in(arg_keys[5], 71), 0),
        "global_blocks": jax.random.randint(arg_keys[4], (GLOBALS,), 0, BLOCKS).astype(jnp.int32),
    }


def reference(query_rows, key_rows, value_rows, random_table, global_blocks):
    grouping = Q_HEADS // KV_HEADS
    score_scale = 1.0 / math.sqrt(HEAD_DIM)
    query_split = query_rows.reshape(BLOCKS, BLOCK, KV_HEADS, grouping, HEAD_DIM)
    key_heads = key_rows.reshape(BLOCKS, BLOCK, KV_HEADS, HEAD_DIM).transpose(2, 0, 1, 3)
    value_heads = value_rows.reshape(BLOCKS, BLOCK, KV_HEADS, HEAD_DIM).transpose(2, 0, 1, 3)
    head_range = jnp.arange(KV_HEADS, dtype=jnp.int32)[:, None]

    def one_block(block_index):
        before = jnp.maximum(block_index - 1, 0)
        following = jnp.minimum(block_index + 1, BLOCKS - 1)
        window = jnp.stack([before, block_index, following]).astype(jnp.int32)
        shared = jnp.concatenate([window, global_blocks.astype(jnp.int32)])
        chosen = jnp.concatenate([jnp.broadcast_to(shared, (KV_HEADS, shared.shape[0])), random_table[block_index].astype(jnp.int32)], axis=1)
        key_sel = key_heads[head_range, chosen].reshape(KV_HEADS, -1, HEAD_DIM)
        value_sel = value_heads[head_range, chosen].reshape(KV_HEADS, -1, HEAD_DIM)
        block_flags = jnp.concatenate([jnp.stack([block_index > 0, block_index >= 0, block_index < BLOCKS - 1]), jnp.ones((GLOBALS + RANDOM,), dtype=bool)])
        usable = jnp.repeat(block_flags, BLOCK)
        scores = jnp.einsum('tkgd,ksd->kgts', query_split[block_index].astype(jnp.float32), key_sel.astype(jnp.float32)) * score_scale
        scores = jnp.where(usable, scores, -1e+30)
        row_max = lax.optimization_barrier(jnp.max(scores, axis=-1, keepdims=True))
        weights = jnp.exp(scores - row_max)
        row_total = lax.optimization_barrier(jnp.sum(weights, axis=-1))
        rounded = weights.astype(jnp.bfloat16)
        mixed = jnp.einsum('kgts,ksd->tkgd', rounded.astype(jnp.float32), value_sel.astype(jnp.float32))
        mixed = mixed / jnp.transpose(row_total, (2, 0, 1))[..., None]
        return mixed.reshape(BLOCK, Q_HEADS * HEAD_DIM).astype(jnp.bfloat16)
    result = lax.map(one_block, jnp.arange(BLOCKS, dtype=jnp.int32))
    return result.reshape(TOKENS, Q_HEADS * HEAD_DIM)
```

```python
import functools
import math

import jax
import jax.numpy as jnp
from jax import lax
from jax.experimental import pallas as pl
from jax.experimental.pallas import tpu as pltpu
from jax.sharding import PartitionSpec as P

BLOCK = 128
HEAD_DIM = 128
GLOBALS = 2
RANDOM = 3
WINDOW = 3
MIB = 2**20


ANY = pl.BlockSpec(memory_space=pl.ANY)
SMEM = pl.BlockSpec(memory_space=pltpu.SMEM)
VMEM = pl.BlockSpec(memory_space=pltpu.VMEM)


def run_copies(copies):
    for copy in copies:
        copy.start()
    for copy in copies:
        copy.wait()


def pack_kernel(heads, order, key_ref, value_ref, *rest):
    outs, (parts, sem_in, sem_out) = rest[:heads], rest[heads:]
    loads = []
    for r in range(heads):
        lanes = pl.ds(pl.multiple_of(order[r] * HEAD_DIM, HEAD_DIM), HEAD_DIM)
        for which, source in enumerate((key_ref, value_ref)):
            loads.append(
                pltpu.make_async_copy(
                    source.at[:, lanes], parts.at[r, which], sem_in.at[r, which]
                )
            )
    for copy in loads:
        copy.start()
    stores = []
    for r in range(heads):
        for which in range(2):
            loads[2 * r + which].wait()
        stores.append(pltpu.make_async_copy(parts.at[r], outs[r], sem_out.at[r]))
        stores[-1].start()
    for copy in stores:
        copy.wait()


def pack(order, key_rows, value_rows):
    rows, columns = key_rows.shape
    heads = columns // HEAD_DIM
    part = jax.ShapeDtypeStruct((2, rows, HEAD_DIM), key_rows.dtype)
    return pl.pallas_call(
        functools.partial(pack_kernel, heads),
        in_specs=[SMEM, ANY, ANY],
        out_specs=[ANY] * heads,
        out_shape=[part] * heads,
        scratch_shapes=[
            pltpu.VMEM((heads, 2, rows, HEAD_DIM), key_rows.dtype),
            pltpu.SemaphoreType.DMA((heads, 2)),
            pltpu.SemaphoreType.DMA((heads,)),
        ],
        compiler_params=pltpu.CompilerParams(vmem_limit_bytes=16 * MIB),
        name="pack",
    )(order, key_rows, value_rows)


def pick_kernel(heads, chunks, slots, order, sources, shared, *rest):
    parts, rest = rest[:heads], rest[heads:]
    outs, shared_ref, (run, sem_in, sem_out) = rest[:chunks], rest[chunks], rest[chunks + 1 :]
    rows = parts[0].shape[1]
    loads = []
    for r in range(heads):
        place = pl.ds(pl.multiple_of(order[r] * rows, BLOCK), rows)
        loads.append(pltpu.make_async_copy(parts[r], run.at[:, place], sem_in.at[r]))
    run_copies(loads)
    stores = []
    for chunk in range(chunks):
        for slot in range(slots):
            place = pl.ds(pl.multiple_of(sources[chunk * slots + slot] * BLOCK, BLOCK), BLOCK)
            stores.append(
                pltpu.make_async_copy(
                    run.at[:, place],
                    outs[chunk].at[:, slot * BLOCK : (slot + 1) * BLOCK],
                    sem_out.at[chunk, slot],
                )
            )
    for copy in stores:
        copy.start()
    for which in range(GLOBALS):
        place = pl.ds(pl.multiple_of(shared[2 * which] * BLOCK, BLOCK), BLOCK)
        block = run[:, place]
        shared_ref[:, which * BLOCK : (which + 1) * BLOCK] = jnp.where(
            shared[2 * which + 1] != 0, block, jnp.zeros_like(block)
        )
    for copy in stores:
        copy.wait()


def pick(order, sources, shared, parts, chunks, slots):
    heads = len(parts)
    rows, dtype = parts[0].shape[1], parts[0].dtype
    return pl.pallas_call(
        functools.partial(pick_kernel, heads, chunks, slots),
        in_specs=[SMEM, SMEM, SMEM] + [ANY] * heads,
        out_specs=[ANY] * chunks + [VMEM],
        out_shape=[jax.ShapeDtypeStruct((2, slots * BLOCK, HEAD_DIM), dtype)] * chunks
        + [jax.ShapeDtypeStruct((2, GLOBALS * BLOCK, HEAD_DIM), dtype)],
        scratch_shapes=[
            pltpu.VMEM((2, heads * rows, HEAD_DIM), dtype),
            pltpu.SemaphoreType.DMA((heads,)),
            pltpu.SemaphoreType.DMA((chunks, slots)),
        ],
        compiler_params=pltpu.CompilerParams(vmem_limit_bytes=24 * MIB),
        name="pick",
    )(order, sources, shared, *parts)


def attend_kernel(layout, grouping, order, table, flags, query_ref, *rest):
    sources, rest = rest[: sum(len(part) for part in layout)], rest[sum(len(part) for part in layout) :]
    out_ref, held, keys, values, sems = rest
    part = pl.program_id(0)
    block = pl.program_id(1)
    listed = WINDOW + GLOBALS + RANDOM

    copies = []
    number = 0
    for r, entries in enumerate(layout):
        mine = []
        for start, lanes, size in entries:
            source = sources[number]
            if lanes:
                for which in range(2):
                    columns = pl.ds(pl.multiple_of(order[r] * HEAD_DIM, HEAD_DIM), HEAD_DIM)
                    mine.append(
                        (source.at[which, :, columns], held.at[r, which, start : start + size])
                    )
            else:
                mine.append((source, held.at[r, :, start : start + size]))
            number += 1
        copies.append(
            [
                pltpu.make_async_copy(src, dst, sems.at[r, place])
                for place, (src, dst) in enumerate(mine)
            ]
        )

    @pl.when((part == 0) & (block == 0))
    def _():
        for group in copies:
            for copy in group:
                copy.start()

    for r, group in enumerate(copies):

        @pl.when((part == r) & (block == 0))
        def _(group=group):
            for copy in group:
                copy.wait()

    base = (part * pl.num_programs(1) + block) * listed
    for entry in range(listed):
        place = pl.ds(pl.multiple_of(table[base + entry] * BLOCK, BLOCK), BLOCK)
        keys[entry * BLOCK : (entry + 1) * BLOCK] = held[part, 0, place]
        values[entry * BLOCK : (entry + 1) * BLOCK] = held[part, 1, place]
    before = flags[2 * block] != 0
    after = flags[2 * block + 1] != 0
    scale = math.log2(math.e) / math.sqrt(HEAD_DIM)
    joined = 2
    for step in range(grouping // joined):
        lanes = [
            slice((step * joined + j) * HEAD_DIM, (step * joined + j + 1) * HEAD_DIM)
            for j in range(joined)
        ]
        query = jnp.concatenate([query_ref[:, lane] for lane in lanes], axis=0)
        scores = lax.dot_general(
            query, keys[...], (((1,), (1,)), ((), ())), preferred_element_type=jnp.float32
        )
        scores = jnp.concatenate(
            [
                jnp.where(before, scores[:, :BLOCK], -1e30),
                scores[:, BLOCK : 2 * BLOCK],
                jnp.where(after, scores[:, 2 * BLOCK : 3 * BLOCK], -1e30),
                scores[:, 3 * BLOCK :],
            ],
            axis=1,
        )
        row_max = jnp.max(scores, axis=1, keepdims=True)
        weights = jnp.exp2((scores - row_max) * scale)
        row_total = jnp.sum(weights, axis=1, keepdims=True)
        mixed = jnp.dot(
            weights.astype(jnp.bfloat16), values[...], preferred_element_type=jnp.float32
        )
        mixed = (mixed * (1.0 / row_total)).astype(out_ref.dtype)
        for j, lane in enumerate(lanes):
            out_ref[:, lane] = mixed[j * BLOCK : (j + 1) * BLOCK]


def attend(order, table, flags, queries, parts, total_rows):
    rows, columns = queries.shape
    width = columns // len(parts)
    blocks = rows // BLOCK
    layout = tuple(
        tuple((start, lanes, array.shape[1]) for start, lanes, array in part) for part in parts
    )
    arrays = [array for part in parts for _, _, array in part]
    most = max(sum(2 if lanes else 1 for _, lanes, _ in part) for part in layout)
    spec = pl.BlockSpec((BLOCK, width), lambda r, i, order, table, flags: (i, order[r]))
    return pl.pallas_call(
        functools.partial(attend_kernel, layout, width // HEAD_DIM),
        grid_spec=pltpu.PrefetchScalarGridSpec(
            num_scalar_prefetch=3,
            grid=(len(parts), blocks),
            in_specs=[spec] + [ANY] * len(arrays),
            out_specs=spec,
            scratch_shapes=[
                pltpu.VMEM((len(parts), 2, total_rows, HEAD_DIM), queries.dtype),
                pltpu.VMEM(((WINDOW + GLOBALS + RANDOM) * BLOCK, HEAD_DIM), queries.dtype),
                pltpu.VMEM(((WINDOW + GLOBALS + RANDOM) * BLOCK, HEAD_DIM), queries.dtype),
                pltpu.SemaphoreType.DMA((len(parts), most)),
            ],
        ),
        out_shape=jax.ShapeDtypeStruct((rows, columns), queries.dtype),
        compiler_params=pltpu.CompilerParams(vmem_limit_bytes=52 * MIB),
        name="attend",
    )(order, table, flags, queries, *arrays)


def plan(random_table, global_blocks, seq_index, head_index, seq_count, heads, my_blocks, slots):
    blocks = random_table.shape[0]
    run_blocks = blocks // seq_count
    by_run = random_table.reshape(seq_count, run_blocks, heads, RANDOM)
    mine = lax.dynamic_index_in_dim(by_run, head_index, 2, keepdims=False)
    mine = mine.reshape(seq_count, run_blocks * RANDOM) - seq_index * run_blocks
    local = jnp.arange(run_blocks, dtype=jnp.int32)
    named = jnp.any(mine[:, None, :] == local[:, None], axis=2)
    rank = jnp.sum(named[:, None, :] & (local[None, :] < local[:, None]), axis=2)
    hit = named[:, None, :] & (rank[:, None, :] == jnp.arange(slots)[:, None])
    sources = jnp.sum(jnp.where(hit, local, 0), axis=2).astype(jnp.int32)
    run = lax.dynamic_index_in_dim(by_run, seq_index, 0, keepdims=False)
    run = run.transpose(1, 0, 2).reshape(heads, run_blocks * RANDOM)
    order_of = jnp.arange(run_blocks * RANDOM)
    earlier = order_of[None, :] < order_of[:, None]
    first = ~jnp.any((run[:, :, None] == run[:, None, :]) & earlier, axis=2)
    start = head_index * my_blocks * RANDOM
    wanted = lax.dynamic_slice_in_dim(run, start, my_blocks * RANDOM, 1)
    same = (wanted[:, :, None] // run_blocks) == (run[:, None, :] // run_blocks)
    below = run[:, None, :] < wanted[:, :, None]
    slot = jnp.sum(same & below & first[:, None, :], axis=2).astype(jnp.int32)
    return sources, wanted // run_blocks, slot


def on_device(query_rows, key_rows, value_rows, random_table, global_blocks):
    seq_count, heads = lax.axis_size("seq"), lax.axis_size("head")
    seq_index, head_index = lax.axis_index("seq"), lax.axis_index("head")
    rows = key_rows.shape[0]
    my_blocks = rows // BLOCK
    run_blocks = my_blocks * heads
    slots = max(1, (RANDOM * run_blocks + 2 * seq_count - 1) // (2 * seq_count))
    order = head_index ^ jnp.arange(heads, dtype=jnp.int32)
    chunk_of = seq_index ^ jnp.arange(seq_count, dtype=jnp.int32)

    parts = pack(order, key_rows, value_rows)

    def across(array, axis, count, bit):
        return lax.ppermute(array, axis, [(i, i ^ bit) for i in range(count)])

    arrived = [parts[0]] + [across(parts[r], "head", heads, r) for r in range(1, heads)]

    flat = seq_count * heads
    edge = jnp.stack([key_rows[rows - BLOCK :], value_rows[rows - BLOCK :]])
    previous = lax.ppermute(edge, ("seq", "head"), [(i, i + 1) for i in range(flat - 1)])
    edge = jnp.stack([key_rows[:BLOCK], value_rows[:BLOCK]])
    upcoming = lax.ppermute(edge, ("seq", "head"), [(i + 1, i) for i in range(flat - 1)])

    sources, owner, slot = plan(
        random_table, global_blocks, seq_index, head_index, seq_count, heads, my_blocks, slots
    )
    sources = jnp.take(sources, chunk_of, axis=0).reshape(-1)
    shared = jnp.stack(
        [global_blocks % run_blocks, (global_blocks // run_blocks == seq_index).astype(jnp.int32)],
        axis=1,
    ).reshape(-1)
    picked = pick(order, sources, shared, arrived, seq_count, slots)
    outgoing, common = picked[:seq_count], picked[seq_count]
    bit = 1
    while bit < seq_count:
        common = common + across(common, "seq", seq_count, bit)
        bit *= 2
    chunks = [outgoing[0]] + [
        across(outgoing[k], "seq", seq_count, k) for k in range(1, seq_count)
    ]
    half = seq_count // 2
    own = [
        jnp.concatenate(chunks[:half], axis=1),
        jnp.concatenate(chunks[half:] + [common], axis=1),
    ]
    held = [own]
    bit = heads // 2
    groups = {0: own}
    while bit:
        for r in sorted(groups):
            groups[r + bit] = [across(array, "head", heads, bit) for array in groups[r]]
        bit //= 2

    local = jnp.arange(my_blocks, dtype=jnp.int32)
    before = jnp.where(local == 0, my_blocks, local - 1)
    after = jnp.where(local == my_blocks - 1, my_blocks + 1, local + 1)
    first_slot = my_blocks + 2
    window = jnp.stack([before, local, after], axis=1)
    commons = first_slot + seq_count * slots + jnp.arange(GLOBALS, dtype=jnp.int32)
    fixed = jnp.concatenate(
        [window, jnp.broadcast_to(commons[None], (my_blocks, GLOBALS))], axis=1
    )
    place = first_slot + (owner ^ seq_index) * slots + slot
    place = jnp.take(place, order, axis=0).reshape(heads, my_blocks, RANDOM)
    table = jnp.concatenate(
        [jnp.broadcast_to(fixed[None], (heads,) + fixed.shape), place], axis=2
    ).reshape(-1)
    number = (seq_index * heads + head_index) * my_blocks + local
    flags = jnp.stack(
        [number > 0, number < seq_count * run_blocks - 1], axis=1
    ).astype(jnp.int32).reshape(-1)
    start_a = first_slot * BLOCK
    start_b = start_a + half * slots * BLOCK
    total_rows = start_b + own[1].shape[1]
    held = [
        [
            (0, False, parts[r]),
            (my_blocks * BLOCK, True, previous),
            ((my_blocks + 1) * BLOCK, True, upcoming),
            (start_a, False, groups[r][0]),
            (start_b, False, groups[r][1]),
        ]
        for r in range(heads)
    ]
    return attend(order, table, flags, query_rows, held, total_rows)


def solution(mesh):
    placed = (
        P(("seq", "head"), None),
        P(("seq", "head"), None),
        P(("seq", "head"), None),
        P(),
        P(),
    )
    return jax.shard_map(
        on_device, mesh=mesh, in_specs=placed, out_specs=P(("seq", "head"), None), check_vma=False
    )
```

```python
import functools
import math

import jax
import jax.numpy as jnp
from jax import lax
from jax.experimental import pallas as pl
from jax.experimental.pallas import tpu as pltpu
from jax.sharding import PartitionSpec as P


BLOCK = 128
HEAD_DIM = 128
GLOBALS = 2
RANDOM = 3
WINDOW = 3
MIB = 2**20
SOME_VMEM = 20 * MIB
MOST_VMEM = 60 * MIB


ANY = pl.BlockSpec(memory_space=pl.ANY)
SMEM = pl.BlockSpec(memory_space=pltpu.SMEM)
VMEM = pl.BlockSpec(memory_space=pltpu.VMEM)


def run_copies(copies):
    for copy in copies:
        copy.start()
    for copy in copies:
        copy.wait()


def pack_kernel(heads, order, key_ref, value_ref, *rest):
    outs, first, last = rest[:heads], rest[heads], rest[heads + 1]
    parts, edges, sem_in, sem_out, sem_edge_in, sem_edge_out = rest[heads + 2 :]
    rows = key_ref.shape[0]
    loads = []
    for r in range(heads):
        lanes = pl.ds(pl.multiple_of(order[r] * HEAD_DIM, HEAD_DIM), HEAD_DIM)
        for which, source in enumerate((key_ref, value_ref)):
            loads.append(
                pltpu.make_async_copy(
                    source.at[:, lanes], parts.at[r, which], sem_in.at[r, which]
                )
            )
    for which, source in enumerate((key_ref, value_ref)):
        for side, start in enumerate((0, rows - BLOCK)):
            loads.append(
                pltpu.make_async_copy(
                    source.at[start : start + BLOCK],
                    edges.at[side, which],
                    sem_edge_in.at[side, which],
                )
            )
    run_copies(loads)
    run_copies(
        [pltpu.make_async_copy(parts.at[r], outs[r], sem_out.at[r]) for r in range(heads)]
        + [
            pltpu.make_async_copy(edges.at[side], out, sem_edge_out.at[side])
            for side, out in enumerate((first, last))
        ]
    )


def pack(order, key_rows, value_rows):
    rows, columns = key_rows.shape
    heads = columns // HEAD_DIM
    part = jax.ShapeDtypeStruct((2, rows, HEAD_DIM), key_rows.dtype)
    edge = jax.ShapeDtypeStruct((2, BLOCK, columns), key_rows.dtype)
    return pl.pallas_call(
        functools.partial(pack_kernel, heads),
        in_specs=[SMEM, ANY, ANY],
        out_specs=[ANY] * (heads + 2),
        out_shape=[part] * heads + [edge] * 2,
        scratch_shapes=[
            pltpu.VMEM((heads, 2, rows, HEAD_DIM), key_rows.dtype),
            pltpu.VMEM((2, 2, BLOCK, columns), key_rows.dtype),
            pltpu.SemaphoreType.DMA((heads, 2)),
            pltpu.SemaphoreType.DMA((heads,)),
            pltpu.SemaphoreType.DMA((2, 2)),
            pltpu.SemaphoreType.DMA((2,)),
        ],
        compiler_params=pltpu.CompilerParams(vmem_limit_bytes=MOST_VMEM),
        name="pack",
    )(order, key_rows, value_rows)


def pick_kernel(heads, chunks, slots, order, sources, shared, *rest):
    parts, rest = rest[:heads], rest[heads:]
    outs, shared_ref, (run, sem_in, sem_out) = rest[:chunks], rest[chunks], rest[chunks + 1 :]
    rows = parts[0].shape[1]
    loads = []
    for r in range(heads):
        place = pl.ds(pl.multiple_of(order[r] * rows, BLOCK), rows)
        loads.append(pltpu.make_async_copy(parts[r], run.at[:, place], sem_in.at[r]))
    run_copies(loads)
    stores = []
    for chunk in range(chunks):
        for slot in range(slots):
            place = pl.ds(pl.multiple_of(sources[chunk * slots + slot] * BLOCK, BLOCK), BLOCK)
            stores.append(
                pltpu.make_async_copy(
                    run.at[:, place],
                    outs[chunk].at[:, slot * BLOCK : (slot + 1) * BLOCK],
                    sem_out.at[chunk, slot],
                )
            )
    for copy in stores:
        copy.start()
    for which in range(GLOBALS):
        place = pl.ds(pl.multiple_of(shared[2 * which] * BLOCK, BLOCK), BLOCK)
        block = run[:, place]
        shared_ref[:, which * BLOCK : (which + 1) * BLOCK] = jnp.where(
            shared[2 * which + 1] != 0, block, jnp.zeros_like(block)
        )
    for copy in stores:
        copy.wait()


def pick(order, sources, shared, parts, chunks, slots):
    heads = len(parts)
    rows, dtype = parts[0].shape[1], parts[0].dtype
    return pl.pallas_call(
        functools.partial(pick_kernel, heads, chunks, slots),
        in_specs=[SMEM, SMEM, SMEM] + [ANY] * heads,
        out_specs=[ANY] * chunks + [VMEM],
        out_shape=[jax.ShapeDtypeStruct((2, slots * BLOCK, HEAD_DIM), dtype)] * chunks
        + [jax.ShapeDtypeStruct((2, GLOBALS * BLOCK, HEAD_DIM), dtype)],
        scratch_shapes=[
            pltpu.VMEM((2, heads * rows, HEAD_DIM), dtype),
            pltpu.SemaphoreType.DMA((heads,)),
            pltpu.SemaphoreType.DMA((chunks, slots)),
        ],
        compiler_params=pltpu.CompilerParams(vmem_limit_bytes=SOME_VMEM),
        name="pick",
    )(order, sources, shared, *parts)


def join_kernel(count, *refs):
    sources, out_ref, sems = refs[:count], refs[count], refs[count + 1]
    copies, start = [], 0
    for place, source in enumerate(sources):
        size = source.shape[1]
        copies.append(
            pltpu.make_async_copy(source, out_ref.at[:, start : start + size], sems.at[place])
        )
        start += size
    run_copies(copies)


def join(arrays):
    rows = sum(array.shape[1] for array in arrays)
    shape = (2, rows, HEAD_DIM)
    return pl.pallas_call(
        functools.partial(join_kernel, len(arrays)),
        in_specs=[ANY] * len(arrays),
        out_specs=VMEM,
        out_shape=jax.ShapeDtypeStruct(shape, arrays[0].dtype),
        scratch_shapes=[pltpu.SemaphoreType.DMA((len(arrays),))],
        compiler_params=pltpu.CompilerParams(vmem_limit_bytes=SOME_VMEM),
        name="join",
    )(*arrays)


def stacked(ref, step, joined):
    first = step * joined
    return jnp.concatenate(
        [ref[:, (first + j) * HEAD_DIM : (first + j + 1) * HEAD_DIM] for j in range(joined)],
        axis=0,
    )


SCALE = math.log2(math.e) / math.sqrt(HEAD_DIM)
JOINED = 2


def window_kernel(parts, grouping, order, flags, query_ref, *rest):
    locals_, (previous, upcoming), rest = rest[:parts], rest[parts : parts + 2], rest[parts + 2 :]
    out_ref, stat_ref, held, sems = rest
    part, block = pl.program_id(0), pl.program_id(1)
    rows = locals_[0].shape[1]
    copies = []
    for r in range(parts):
        columns = pl.ds(pl.multiple_of(order[r] * HEAD_DIM, HEAD_DIM), HEAD_DIM)
        pairs = [(locals_[r], held.at[r, :, BLOCK : BLOCK + rows])]
        for which in range(2):
            pairs.append((previous.at[which, :, columns], held.at[r, which, :BLOCK]))
            pairs.append((upcoming.at[which, :, columns], held.at[r, which, BLOCK + rows :]))
        copies.append(
            [
                pltpu.make_async_copy(src, dst, sems.at[r, place])
                for place, (src, dst) in enumerate(pairs)
            ]
        )

    @pl.when((part == 0) & (block == 0))
    def _():
        for group in copies:
            for copy in group:
                copy.start()

    for r, group in enumerate(copies):

        @pl.when((part == r) & (block == 0))
        def _(group=group):
            for copy in group:
                copy.wait()

    place = pl.ds(pl.multiple_of(block * BLOCK, BLOCK), WINDOW * BLOCK)
    keys, values = held[part, 0, place], held[part, 1, place]
    before, after = flags[2 * block] != 0, flags[2 * block + 1] != 0
    lane = lax.broadcasted_iota(jnp.int32, (BLOCK, HEAD_DIM), 1)
    stats = jnp.zeros((BLOCK, HEAD_DIM), jnp.float32)
    for step in range(grouping // JOINED):
        scores = lax.dot_general(
            stacked(query_ref, step, JOINED),
            keys,
            (((1,), (1,)), ((), ())),
            preferred_element_type=jnp.float32,
        )
        scores = jnp.concatenate(
            [
                jnp.where(before, scores[:, :BLOCK], -1e30),
                scores[:, BLOCK : 2 * BLOCK],
                jnp.where(after, scores[:, 2 * BLOCK :], -1e30),
            ],
            axis=1,
        )
        row_max = jnp.max(scores, axis=1, keepdims=True)
        weights = jnp.exp2((scores - row_max) * SCALE)
        row_total = jnp.sum(weights, axis=1, keepdims=True)
        mixed = jnp.dot(
            weights.astype(values.dtype), values, preferred_element_type=jnp.float32
        )
        for j in range(JOINED):
            head = step * JOINED + j
            some = slice(j * BLOCK, (j + 1) * BLOCK)
            out_ref[0, :, head * HEAD_DIM : (head + 1) * HEAD_DIM] = mixed[some]
            stats = jnp.where(lane == head, row_max[some], stats)
            stats = jnp.where(lane == grouping + head, row_total[some], stats)
    stat_ref[0, 0] = stats


def window_share(order, flags, queries, locals_, previous, upcoming):
    rows, columns = queries.shape
    heads = previous.shape[2] // HEAD_DIM
    width = columns // heads
    blocks = rows // BLOCK
    parts = len(locals_)
    pairs = parts * blocks * (width // HEAD_DIM) * BLOCK * WINDOW * BLOCK
    return pl.pallas_call(
        functools.partial(window_kernel, parts, width // HEAD_DIM),
        grid_spec=pltpu.PrefetchScalarGridSpec(
            num_scalar_prefetch=2,
            grid=(parts, blocks),
            in_specs=[pl.BlockSpec((BLOCK, width), lambda r, i, order, flags: (i, order[r]))]
            + [ANY] * (parts + 2),
            out_specs=[
                pl.BlockSpec((1, BLOCK, width), lambda r, i, order, flags: (r, i, 0)),
                pl.BlockSpec((1, 1, BLOCK, HEAD_DIM), lambda r, i, order, flags: (r, i, 0, 0)),
            ],
            scratch_shapes=[
                pltpu.VMEM((parts, 2, rows + 2 * BLOCK, HEAD_DIM), queries.dtype),
                pltpu.SemaphoreType.DMA((parts, 5)),
            ],
        ),
        out_shape=[
            jax.ShapeDtypeStruct((parts, rows, width), jnp.float32),
            jax.ShapeDtypeStruct((parts, blocks, BLOCK, HEAD_DIM), jnp.float32),
        ],
        compiler_params=pltpu.CompilerParams(vmem_limit_bytes=MOST_VMEM),
        cost_estimate=pl.CostEstimate(
            flops=4 * pairs * HEAD_DIM, bytes_accessed=8 * MIB, transcendentals=pairs
        ),
        name="window",
    )(order, flags, queries, *locals_, previous, upcoming)


def finish_kernel(sizes, grouping, aliased, order, table, query_ref, mixed_ref, stat_ref, *rest):
    parts = len(sizes)
    flat = [size for part in sizes for size in part]
    sources, rest = rest[: len(flat)], rest[len(flat) + aliased :]
    out_ref, held, keys, values, sems = rest
    part, block = pl.program_id(0), pl.program_id(1)
    listed = GLOBALS + RANDOM
    copies = []
    number = 0
    for r in range(parts):
        group, start = [], 0
        for place, size in enumerate(sizes[r]):
            group.append(
                pltpu.make_async_copy(
                    sources[number], held.at[r, :, start : start + size], sems.at[r, place]
                )
            )
            start += size
            number += 1
        copies.append(group)

    @pl.when((part == 0) & (block == 0))
    def _():
        for group in copies:
            for copy in group:
                copy.start()

    for r, group in enumerate(copies):

        @pl.when((part == r) & (block == 0))
        def _(group=group):
            for copy in group:
                copy.wait()

    base = (part * pl.num_programs(1) + block) * listed
    for entry in range(listed):
        place = pl.ds(pl.multiple_of(table[base + entry] * BLOCK, BLOCK), BLOCK)
        keys[entry * BLOCK : (entry + 1) * BLOCK] = held[part, 0, place]
        values[entry * BLOCK : (entry + 1) * BLOCK] = held[part, 1, place]
    stats = stat_ref[0, 0]
    for step in range(grouping // JOINED):
        first = step * JOINED
        old_max = jnp.concatenate(
            [stats[:, first + j : first + j + 1] for j in range(JOINED)], axis=0
        )
        old_total = jnp.concatenate(
            [stats[:, grouping + first + j : grouping + first + j + 1] for j in range(JOINED)],
            axis=0,
        )
        scores = lax.dot_general(
            stacked(query_ref, step, JOINED),
            keys[...],
            (((1,), (1,)), ((), ())),
            preferred_element_type=jnp.float32,
        )
        row_max = jnp.maximum(old_max, jnp.max(scores, axis=1, keepdims=True))
        weights = jnp.exp2((scores - row_max) * SCALE)
        kept = jnp.exp2((old_max - row_max) * SCALE)
        row_total = old_total * kept + jnp.sum(weights, axis=1, keepdims=True)
        mixed = jnp.dot(
            weights.astype(values.dtype), values[...], preferred_element_type=jnp.float32
        )
        inverse = 1.0 / row_total
        kept = kept * inverse
        for j in range(JOINED):
            lanes = slice((first + j) * HEAD_DIM, (first + j + 1) * HEAD_DIM)
            some = slice(j * BLOCK, (j + 1) * BLOCK)
            total = mixed[some] * inverse[some] + mixed_ref[0, :, lanes] * kept[some]
            out_ref[:, lanes] = total.astype(out_ref.dtype)


def finish(order, table, queries, share, parts, start, output):
    rows, columns = queries.shape
    width = share[0].shape[2]
    blocks = rows // BLOCK
    sizes = tuple(tuple(array.shape[1] for array in part) for part in parts)
    arrays = [array for part in parts for array in part]
    listed = GLOBALS + RANDOM
    pairs = len(parts) * blocks * (width // HEAD_DIM) * BLOCK * listed * BLOCK
    spec = pl.BlockSpec((BLOCK, width), lambda r, i, order, table: (i, order[r]))
    aliased = [] if output is None else [output]
    operands = (order, table, queries, *share, *arrays, *aliased)
    return pl.pallas_call(
        functools.partial(finish_kernel, sizes, width // HEAD_DIM, len(aliased)),
        grid_spec=pltpu.PrefetchScalarGridSpec(
            num_scalar_prefetch=2,
            grid=(len(parts), blocks),
            in_specs=[
                spec,
                pl.BlockSpec((1, BLOCK, width), lambda r, i, order, table: (r + start, i, 0)),
                pl.BlockSpec(
                    (1, 1, BLOCK, HEAD_DIM), lambda r, i, order, table: (r + start, i, 0, 0)
                ),
            ]
            + [ANY] * (len(arrays) + len(aliased)),
            out_specs=spec,
            scratch_shapes=[
                pltpu.VMEM((len(parts), 2, sum(sizes[0]), HEAD_DIM), queries.dtype),
                pltpu.VMEM((listed * BLOCK, HEAD_DIM), queries.dtype),
                pltpu.VMEM((listed * BLOCK, HEAD_DIM), queries.dtype),
                pltpu.SemaphoreType.DMA((len(parts), len(sizes[0]))),
            ],
        ),
        out_shape=jax.ShapeDtypeStruct((rows, columns), queries.dtype),
        input_output_aliases={len(operands) - 1: 0} if aliased else {},
        compiler_params=pltpu.CompilerParams(vmem_limit_bytes=MOST_VMEM),
        cost_estimate=pl.CostEstimate(
            flops=4 * pairs * HEAD_DIM, bytes_accessed=8 * MIB, transcendentals=pairs
        ),
        name="finish",
    )(*operands)


def plan(random_table, seq_index, head_index, seq_count, heads, my_blocks, slots):
    blocks = random_table.shape[0]
    run_blocks = blocks // seq_count
    by_run = random_table.reshape(seq_count, run_blocks, heads, RANDOM)
    mine = lax.dynamic_index_in_dim(by_run, head_index, 2, keepdims=False)
    mine = mine.reshape(seq_count, run_blocks * RANDOM) - seq_index * run_blocks
    local = jnp.arange(run_blocks, dtype=jnp.int32)
    named = jnp.any(mine[:, None, :] == local[:, None], axis=2)
    rank = jnp.sum(named[:, None, :] & (local[None, :] < local[:, None]), axis=2)
    hit = named[:, None, :] & (rank[:, None, :] == jnp.arange(slots)[:, None])
    sources = jnp.sum(jnp.where(hit, local, 0), axis=2).astype(jnp.int32)
    run = lax.dynamic_index_in_dim(by_run, seq_index, 0, keepdims=False)
    run = run.transpose(1, 0, 2).reshape(heads, run_blocks * RANDOM)
    order_of = jnp.arange(run_blocks * RANDOM)
    earlier = order_of[None, :] < order_of[:, None]
    first = ~jnp.any((run[:, :, None] == run[:, None, :]) & earlier, axis=2)
    start = head_index * my_blocks * RANDOM
    wanted = lax.dynamic_slice_in_dim(run, start, my_blocks * RANDOM, 1)
    same = (wanted[:, :, None] // run_blocks) == (run[:, None, :] // run_blocks)
    below = run[:, None, :] < wanted[:, :, None]
    slot = jnp.sum(same & below & first[:, None, :], axis=2).astype(jnp.int32)
    return sources, wanted // run_blocks, slot


def on_device(query_rows, key_rows, value_rows, random_table, global_blocks):
    seq_count, heads = lax.axis_size("seq"), lax.axis_size("head")
    seq_index, head_index = lax.axis_index("seq"), lax.axis_index("head")
    rows = key_rows.shape[0]
    my_blocks = rows // BLOCK
    run_blocks = my_blocks * heads
    slots = max(1, (RANDOM * run_blocks + 2 * seq_count - 1) // (2 * seq_count))
    order = head_index ^ jnp.arange(heads, dtype=jnp.int32)
    chunk_of = seq_index ^ jnp.arange(seq_count, dtype=jnp.int32)

    def across(array, axis, bit):
        count = lax.axis_size(axis)
        return lax.ppermute(array, axis, [(i, i ^ bit) for i in range(count)])

    *parts, first, last = pack(order, key_rows, value_rows)
    arrived = [parts[0]] + [across(parts[r], "head", r) for r in range(heads - 1, 0, -1)][::-1]

    flat = seq_count * heads
    previous = lax.ppermute(last, ("seq", "head"), [(i, i + 1) for i in range(flat - 1)])
    upcoming = lax.ppermute(first, ("seq", "head"), [(i + 1, i) for i in range(flat - 1)])

    sources, owner, slot = plan(
        random_table, seq_index, head_index, seq_count, heads, my_blocks, slots
    )
    sources = jnp.take(sources, chunk_of, axis=0).reshape(-1)
    shared = jnp.stack(
        [global_blocks % run_blocks, (global_blocks // run_blocks == seq_index).astype(jnp.int32)],
        axis=1,
    ).reshape(-1)
    picked = pick(order, sources, shared, arrived, seq_count, slots)
    outgoing, common = picked[:seq_count], picked[seq_count]
    chunks = [outgoing[0]] + [across(outgoing[k], "seq", k) for k in range(1, seq_count)]
    bit = 1
    while bit < seq_count:
        common = common + across(common, "seq", bit)
        bit *= 2
    half, last_part = seq_count // 2, (seq_count + seq_count // 2) // 2
    own = [
        chunks[0],
        join(chunks[1:half]),
        join(chunks[half:last_part] + [common]),
        join(chunks[last_part:]),
    ]
    groups = {0: own}
    bit = heads // 2
    while bit:
        for r in sorted(groups):
            groups[r + bit] = [across(array, "head", bit) for array in groups[r]]
        bit //= 2

    local = jnp.arange(my_blocks, dtype=jnp.int32)
    chunk = owner ^ seq_index
    place = chunk * slots + slot + jnp.where(chunk >= last_part, GLOBALS, 0)
    place = jnp.take(place, order, axis=0).reshape(heads, my_blocks, RANDOM)
    commons = last_part * slots + jnp.arange(GLOBALS, dtype=jnp.int32)
    commons = jnp.broadcast_to(commons, (heads, my_blocks, GLOBALS))
    table = jnp.concatenate([commons, place], axis=2).reshape(heads, -1)
    number = (seq_index * heads + head_index) * my_blocks + local
    flags = (
        jnp.stack([number > 0, number < seq_count * run_blocks - 1], axis=1)
        .astype(jnp.int32)
        .reshape(-1)
    )
    half_heads = heads // 2
    shares = []
    for some in (slice(0, half_heads), slice(half_heads, heads)):
        shares.append(window_share(order[some], flags, query_rows, parts[some], previous, upcoming))
    output = None
    pieces = [(0, 0, half_heads)] + [(1, r, r + 1) for r in range(half_heads, heads)]
    for share, begin, end in pieces:
        output = finish(
            order[begin:end],
            table[begin:end].reshape(-1),
            query_rows,
            shares[share],
            [groups[r] for r in range(begin, end)],
            begin - share * half_heads,
            output,
        )
    return output


def solution(mesh):
    placed = (
        P(("seq", "head"), None),
        P(("seq", "head"), None),
        P(("seq", "head"), None),
        P(),
        P(),
    )

    return jax.shard_map(
        on_device, mesh=mesh, in_specs=placed, out_specs=P(("seq", "head"), None), check_vma=False
    )
```

```python
import functools
import math

import jax
import jax.numpy as jnp
from jax import lax
from jax.experimental import pallas as pl
from jax.experimental.pallas import tpu as pltpu
from jax.sharding import PartitionSpec as P


BLOCK = 128
HEAD_DIM = 128
GLOBALS = 2
RANDOM = 3
WINDOW = 3
MIB = 2**20
SOME_VMEM = 20 * MIB
MOST_VMEM = 60 * MIB


ANY = pl.BlockSpec(memory_space=pl.ANY)
SMEM = pl.BlockSpec(memory_space=pltpu.SMEM)
VMEM = pl.BlockSpec(memory_space=pltpu.VMEM)


def run_copies(copies):
    for copy in copies:
        copy.start()
    for copy in copies:
        copy.wait()


def pack_kernel(heads, order, key_ref, value_ref, *rest):
    outs, first, last = rest[:heads], rest[heads], rest[heads + 1]
    parts, edges, sem_in, sem_out, sem_edge_in, sem_edge_out = rest[heads + 2 :]
    rows = key_ref.shape[0]
    loads = []
    for r in range(heads):
        lanes = pl.ds(pl.multiple_of(order[r] * HEAD_DIM, HEAD_DIM), HEAD_DIM)
        for which, source in enumerate((key_ref, value_ref)):
            loads.append(
                pltpu.make_async_copy(
                    source.at[:, lanes], parts.at[r, which], sem_in.at[r, which]
                )
            )
    for which, source in enumerate((key_ref, value_ref)):
        for side, start in enumerate((0, rows - BLOCK)):
            loads.append(
                pltpu.make_async_copy(
                    source.at[start : start + BLOCK],
                    edges.at[side, which],
                    sem_edge_in.at[side, which],
                )
            )
    run_copies(loads)
    run_copies(
        [pltpu.make_async_copy(parts.at[r], outs[r], sem_out.at[r]) for r in range(heads)]
        + [
            pltpu.make_async_copy(edges.at[side], out, sem_edge_out.at[side])
            for side, out in enumerate((first, last))
        ]
    )


def pack(order, key_rows, value_rows):
    rows, columns = key_rows.shape
    heads = columns // HEAD_DIM
    part = jax.ShapeDtypeStruct((2, rows, HEAD_DIM), key_rows.dtype)
    edge = jax.ShapeDtypeStruct((2, BLOCK, columns), key_rows.dtype)
    return pl.pallas_call(
        functools.partial(pack_kernel, heads),
        in_specs=[SMEM, ANY, ANY],
        out_specs=[ANY] * (heads + 2),
        out_shape=[part] * heads + [edge] * 2,
        scratch_shapes=[
            pltpu.VMEM((heads, 2, rows, HEAD_DIM), key_rows.dtype),
            pltpu.VMEM((2, 2, BLOCK, columns), key_rows.dtype),
            pltpu.SemaphoreType.DMA((heads, 2)),
            pltpu.SemaphoreType.DMA((heads,)),
            pltpu.SemaphoreType.DMA((2, 2)),
            pltpu.SemaphoreType.DMA((2,)),
        ],
        compiler_params=pltpu.CompilerParams(vmem_limit_bytes=MOST_VMEM),
        name="pack",
    )(order, key_rows, value_rows)


def pick_kernel(heads, chunks, slots, order, sources, shared, *rest):
    parts, rest = rest[:heads], rest[heads:]
    outs, shared_ref, (run, sem_in, sem_out) = rest[:chunks], rest[chunks], rest[chunks + 1 :]
    rows = parts[0].shape[1]
    loads = []
    for r in range(heads):
        place = pl.ds(pl.multiple_of(order[r] * rows, BLOCK), rows)
        loads.append(pltpu.make_async_copy(parts[r], run.at[:, place], sem_in.at[r]))
    run_copies(loads)
    stores = []
    for chunk in range(chunks):
        for slot in range(slots):
            place = pl.ds(pl.multiple_of(sources[chunk * slots + slot] * BLOCK, BLOCK), BLOCK)
            stores.append(
                pltpu.make_async_copy(
                    run.at[:, place],
                    outs[chunk].at[:, slot * BLOCK : (slot + 1) * BLOCK],
                    sem_out.at[chunk, slot],
                )
            )
    for copy in stores:
        copy.start()
    for which in range(GLOBALS):
        place = pl.ds(pl.multiple_of(shared[2 * which] * BLOCK, BLOCK), BLOCK)
        block = run[:, place]
        shared_ref[:, which * BLOCK : (which + 1) * BLOCK] = jnp.where(
            shared[2 * which + 1] != 0, block, jnp.zeros_like(block)
        )
    for copy in stores:
        copy.wait()


def pick(order, sources, shared, parts, chunks, slots):
    heads = len(parts)
    rows, dtype = parts[0].shape[1], parts[0].dtype
    return pl.pallas_call(
        functools.partial(pick_kernel, heads, chunks, slots),
        in_specs=[SMEM, SMEM, SMEM] + [ANY] * heads,
        out_specs=[ANY] * chunks + [VMEM],
        out_shape=[jax.ShapeDtypeStruct((2, slots * BLOCK, HEAD_DIM), dtype)] * chunks
        + [jax.ShapeDtypeStruct((2, GLOBALS * BLOCK, HEAD_DIM), dtype)],
        scratch_shapes=[
            pltpu.VMEM((2, heads * rows, HEAD_DIM), dtype),
            pltpu.SemaphoreType.DMA((heads,)),
            pltpu.SemaphoreType.DMA((chunks, slots)),
        ],
        compiler_params=pltpu.CompilerParams(vmem_limit_bytes=SOME_VMEM),
        name="pick",
    )(order, sources, shared, *parts)


def join_kernel(count, *refs):
    sources, out_ref, sems = refs[:count], refs[count], refs[count + 1]
    copies, start = [], 0
    for place, source in enumerate(sources):
        size = source.shape[1]
        copies.append(
            pltpu.make_async_copy(source, out_ref.at[:, start : start + size], sems.at[place])
        )
        start += size
    run_copies(copies)


def join(arrays):
    rows = sum(array.shape[1] for array in arrays)
    shape = (2, rows, HEAD_DIM)
    return pl.pallas_call(
        functools.partial(join_kernel, len(arrays)),
        in_specs=[ANY] * len(arrays),
        out_specs=VMEM,
        out_shape=jax.ShapeDtypeStruct(shape, arrays[0].dtype),
        scratch_shapes=[pltpu.SemaphoreType.DMA((len(arrays),))],
        compiler_params=pltpu.CompilerParams(vmem_limit_bytes=SOME_VMEM),
        name="join",
    )(*arrays)


SCALE = math.log2(math.e) / math.sqrt(HEAD_DIM)
JOINED = 2
TOGETHER = 2


def stacked(ref, rows, head):
    return jnp.concatenate(
        [ref[rows, (head + j) * HEAD_DIM : (head + j + 1) * HEAD_DIM] for j in range(JOINED)],
        axis=0,
    )


def score_block(query, keys):
    return lax.dot_general(
        query, keys, (((1,), (1,)), ((), ())), preferred_element_type=jnp.float32
    )


def weighted(scores, top, values):
    weights = jnp.concatenate(
        [
            jnp.exp2((scores[:, start : start + HEAD_DIM] - top) * SCALE)
            for start in range(0, scores.shape[1], HEAD_DIM)
        ],
        axis=1,
    )
    both = jnp.concatenate([values, jnp.ones_like(values)], axis=1)
    mixed = jnp.dot(weights.astype(values.dtype), both, preferred_element_type=jnp.float32)
    return mixed[:, :HEAD_DIM], mixed[:, HEAD_DIM:]


def pipelined(tasks, scores_of, rest_of):
    scores = scores_of(*tasks[0])
    for place, task in enumerate(tasks):
        upcoming = scores_of(*tasks[place + 1]) if place + 1 < len(tasks) else None
        rest_of(*task, scores)
        scores = upcoming


def window_kernel(parts, order, flags, query_ref, *rest):
    locals_, (before_ref, after_ref), rest = rest[:parts], rest[parts : parts + 2], rest[parts + 2 :]
    out_ref, level_ref, held = rest
    part, step = pl.program_id(0), pl.program_id(1)
    _, width = query_ref.shape
    grouping = width // HEAD_DIM
    inner = locals_[0].shape[1]
    for r in range(parts):

        @pl.when((part == r) & (step == 0))
        def _(r=r):
            held[:, BLOCK : BLOCK + inner] = locals_[r][...]
            held[:, :BLOCK] = before_ref[...]
            held[:, BLOCK + inner :] = after_ref[...]

    def listed(which, unit):
        place = pl.ds(pl.multiple_of((step * TOGETHER + unit) * BLOCK, BLOCK), WINDOW * BLOCK)
        return held[which, place]

    def scores_of(unit, head):
        block = step * TOGETHER + unit
        scores = score_block(
            stacked(query_ref, slice(unit * BLOCK, (unit + 1) * BLOCK), head), listed(0, unit)
        )
        return jnp.concatenate(
            [
                jnp.where(flags[2 * block] != 0, scores[:, :BLOCK], -1e30),
                scores[:, BLOCK : 2 * BLOCK],
                jnp.where(flags[2 * block + 1] != 0, scores[:, 2 * BLOCK :], -1e30),
            ],
            axis=1,
        )

    def rest_of(unit, head, scores):
        top = jnp.broadcast_to(
            jnp.max(scores, axis=1, keepdims=True), (scores.shape[0], HEAD_DIM)
        )
        mixed, total = weighted(scores, top, listed(1, unit))
        mixed = mixed * (1.0 / total)
        level = top + jnp.log(total) * math.sqrt(HEAD_DIM)
        for j in range(JOINED):
            some = slice(j * BLOCK, (j + 1) * BLOCK)
            rows = slice(unit * BLOCK, (unit + 1) * BLOCK)
            lanes = slice((head + j) * HEAD_DIM, (head + j + 1) * HEAD_DIM)
            out_ref[0, rows, lanes] = mixed[some]
            level_ref[0, rows, lanes] = level[some]

    tasks = [(unit, head) for unit in range(TOGETHER) for head in range(0, grouping, JOINED)]
    pipelined(tasks, scores_of, rest_of)


def whole_block(array):
    return pl.BlockSpec(array.shape, lambda *_: (0,) * array.ndim)


def window_share(order, flags, queries, locals_, edges):
    rows, columns = queries.shape
    heads = edges[0].shape[2] // HEAD_DIM
    width = columns // heads
    blocks = rows // BLOCK
    parts = len(locals_)
    pairs = parts * blocks * (width // HEAD_DIM) * BLOCK * WINDOW * BLOCK
    some = TOGETHER * BLOCK
    edge = pl.BlockSpec((2, BLOCK, HEAD_DIM), lambda r, i, order, flags: (0, 0, order[r]))
    return pl.pallas_call(
        functools.partial(window_kernel, parts),
        grid_spec=pltpu.PrefetchScalarGridSpec(
            num_scalar_prefetch=2,
            grid=(parts, blocks // TOGETHER),
            in_specs=[pl.BlockSpec((some, width), lambda r, i, order, flags: (i, order[r]))]
            + [whole_block(array) for array in locals_]
            + [edge, edge],
            out_specs=[pl.BlockSpec((1, some, width), lambda r, i, order, flags: (r, i, 0))] * 2,
            scratch_shapes=[pltpu.VMEM((2, rows + 2 * BLOCK, HEAD_DIM), queries.dtype)],
        ),
        out_shape=[jax.ShapeDtypeStruct((parts, rows, width), jnp.float32)] * 2,
        compiler_params=pltpu.CompilerParams(vmem_limit_bytes=MOST_VMEM),
        cost_estimate=pl.CostEstimate(
            flops=4 * pairs * HEAD_DIM, bytes_accessed=8 * MIB, transcendentals=pairs
        ),
        name="window",
    )(order, flags, queries, *locals_, *edges)


LISTED = GLOBALS + RANDOM


def finish_kernel(counts, aliased, order, table, query_ref, mixed_ref, level_ref, *rest):
    sources, (out_ref, held) = rest[: sum(counts)], rest[sum(counts) + aliased :]
    part, step = pl.program_id(0), pl.program_id(1)
    grouping = query_ref.shape[1] // HEAD_DIM
    number = 0
    for r, count in enumerate(counts):

        @pl.when((part == r) & (step == 0))
        def _(mine=sources[number : number + count]):
            start = 0
            for source in mine:
                held[:, start : start + source.shape[1]] = source[...]
                start += source.shape[1]

        number += count
    base = (part * pl.num_programs(1) + step) * TOGETHER * LISTED

    def listed(which, unit):
        return jnp.concatenate(
            [
                held[
                    which,
                    pl.ds(pl.multiple_of(table[base + unit * LISTED + n] * BLOCK, BLOCK), BLOCK),
                ]
                for n in range(LISTED)
            ],
            axis=0,
        )

    def scores_of(unit, head):
        return score_block(
            stacked(query_ref, slice(unit * BLOCK, (unit + 1) * BLOCK), head), listed(0, unit)
        )

    def rest_of(unit, head, scores):
        rows = slice(unit * BLOCK, (unit + 1) * BLOCK)
        level = stacked(level_ref.at[0], rows, head)
        top = jnp.maximum(level, jnp.max(scores, axis=1, keepdims=True))
        mixed, total = weighted(scores, top, listed(1, unit))
        kept = jnp.exp2((level - top) * SCALE)
        inverse = 1.0 / (total + kept)
        mixed = (mixed + stacked(mixed_ref.at[0], rows, head) * kept) * inverse
        for j in range(JOINED):
            lanes = slice((head + j) * HEAD_DIM, (head + j + 1) * HEAD_DIM)
            out_ref[rows, lanes] = mixed[j * BLOCK : (j + 1) * BLOCK].astype(out_ref.dtype)

    tasks = [(unit, head) for unit in range(TOGETHER) for head in range(0, grouping, JOINED)]
    pipelined(tasks, scores_of, rest_of)


def finish(order, table, queries, share, parts, output):
    rows, columns = queries.shape
    width = share[0].shape[2]
    blocks = rows // BLOCK
    arrays = [array for part in parts for array in part]
    pairs = len(parts) * blocks * (width // HEAD_DIM) * BLOCK * LISTED * BLOCK
    some = TOGETHER * BLOCK
    spec = pl.BlockSpec((some, width), lambda r, i, order, table: (i, order[r]))
    aliased = [] if output is None else [output]
    operands = (order, table, queries, *share, *arrays, *aliased)
    return pl.pallas_call(
        functools.partial(finish_kernel, [len(part) for part in parts], len(aliased)),
        grid_spec=pltpu.PrefetchScalarGridSpec(
            num_scalar_prefetch=2,
            grid=(len(parts), blocks // TOGETHER),
            in_specs=[
                spec,
            ]
            + [pl.BlockSpec((1, some, width), lambda r, i, order, table: (r, i, 0))] * 2
            + [whole_block(array) for array in arrays]
            + [ANY] * len(aliased),
            out_specs=spec,
            scratch_shapes=[
                pltpu.VMEM(
                    (2, sum(array.shape[1] for array in parts[0]), HEAD_DIM), queries.dtype
                ),
            ],
        ),
        out_shape=jax.ShapeDtypeStruct((rows, columns), queries.dtype),
        input_output_aliases={len(operands) - 1: 0} if aliased else {},
        compiler_params=pltpu.CompilerParams(vmem_limit_bytes=MOST_VMEM),
        cost_estimate=pl.CostEstimate(
            flops=4 * pairs * HEAD_DIM, bytes_accessed=8 * MIB, transcendentals=pairs
        ),
        name="finish",
    )(*operands)


def plan(random_table, seq_index, head_index, seq_count, heads, my_blocks, slots):
    blocks = random_table.shape[0]
    run_blocks = blocks // seq_count
    by_run = random_table.reshape(seq_count, run_blocks, heads, RANDOM)
    mine = lax.dynamic_index_in_dim(by_run, head_index, 2, keepdims=False)
    mine = mine.reshape(seq_count, run_blocks * RANDOM) - seq_index * run_blocks
    local = jnp.arange(run_blocks, dtype=jnp.int32)
    named = jnp.any(mine[:, None, :] == local[:, None], axis=2)
    rank = jnp.sum(named[:, None, :] & (local[None, :] < local[:, None]), axis=2)
    hit = named[:, None, :] & (rank[:, None, :] == jnp.arange(slots)[:, None])
    sources = jnp.sum(jnp.where(hit, local, 0), axis=2).astype(jnp.int32)
    run = lax.dynamic_index_in_dim(by_run, seq_index, 0, keepdims=False)
    run = run.transpose(1, 0, 2).reshape(heads, run_blocks * RANDOM)
    order_of = jnp.arange(run_blocks * RANDOM)
    earlier = order_of[None, :] < order_of[:, None]
    first = ~jnp.any((run[:, :, None] == run[:, None, :]) & earlier, axis=2)
    start = head_index * my_blocks * RANDOM
    wanted = lax.dynamic_slice_in_dim(run, start, my_blocks * RANDOM, 1)
    same = (wanted[:, :, None] // run_blocks) == (run[:, None, :] // run_blocks)
    below = run[:, None, :] < wanted[:, :, None]
    slot = jnp.sum(same & below & first[:, None, :], axis=2).astype(jnp.int32)
    return sources, wanted // run_blocks, slot


def on_device(query_rows, key_rows, value_rows, random_table, global_blocks):
    seq_count, heads = lax.axis_size("seq"), lax.axis_size("head")
    seq_index, head_index = lax.axis_index("seq"), lax.axis_index("head")
    rows = key_rows.shape[0]
    my_blocks = rows // BLOCK
    run_blocks = my_blocks * heads
    slots = max(1, (RANDOM * run_blocks + 2 * seq_count - 1) // (2 * seq_count))
    order = head_index ^ jnp.arange(heads, dtype=jnp.int32)
    chunk_of = seq_index ^ jnp.arange(seq_count, dtype=jnp.int32)

    def across(array, axis, bit):
        count = lax.axis_size(axis)
        return lax.ppermute(array, axis, [(i, i ^ bit) for i in range(count)])

    *parts, first, last = pack(order, key_rows, value_rows)
    arrived = [parts[0]] + [across(parts[r], "head", r) for r in range(heads - 1, 0, -1)][::-1]

    flat = seq_count * heads
    previous = lax.ppermute(last, ("seq", "head"), [(i, i + 1) for i in range(flat - 1)])
    upcoming = lax.ppermute(first, ("seq", "head"), [(i + 1, i) for i in range(flat - 1)])

    sources, owner, slot = plan(
        random_table, seq_index, head_index, seq_count, heads, my_blocks, slots
    )
    sources = jnp.take(sources, chunk_of, axis=0).reshape(-1)
    shared = jnp.stack(
        [global_blocks % run_blocks, (global_blocks // run_blocks == seq_index).astype(jnp.int32)],
        axis=1,
    ).reshape(-1)
    picked = pick(order, sources, shared, arrived, seq_count, slots)
    outgoing, common = picked[:seq_count], picked[seq_count]
    chunks = [outgoing[0]] + [across(outgoing[k], "seq", k) for k in range(1, seq_count)]
    bit = seq_count // 2
    while bit:
        common = common + across(common, "seq", bit)
        bit //= 2
    half, last_part = seq_count // 2, (seq_count + seq_count // 2) // 2
    own = [
        chunks[0],
        join(chunks[1:half]),
        join([common] + chunks[half:last_part]),
        join(chunks[last_part:]),
    ]
    groups = {0: own}
    bit = heads // 2
    while bit:
        for r in sorted(groups):
            groups[r + bit] = [across(array, "head", bit) for array in groups[r]]
        bit //= 2

    local = jnp.arange(my_blocks, dtype=jnp.int32)
    chunk = owner ^ seq_index
    place = chunk * slots + slot + jnp.where(chunk >= half, GLOBALS, 0)
    place = jnp.take(place, order, axis=0).reshape(heads, my_blocks, RANDOM)
    commons = half * slots + jnp.arange(GLOBALS, dtype=jnp.int32)
    commons = jnp.broadcast_to(commons, (heads, my_blocks, GLOBALS))
    table = jnp.concatenate([commons, place], axis=2).reshape(heads, -1)
    number = (seq_index * heads + head_index) * my_blocks + local
    flags = (
        jnp.stack([number > 0, number < seq_count * run_blocks - 1], axis=1)
        .astype(jnp.int32)
        .reshape(-1)
    )
    half_heads = heads // 2
    shares = []
    for some in (slice(0, half_heads), slice(half_heads, heads)):
        shares.append(
            window_share(
                order[some],
                flags,
                query_rows,
                parts[some],
                (previous, upcoming),
            )
        )
    output = None
    for n, (begin, end) in enumerate(((0, half_heads), (half_heads, heads))):
        output = finish(
            order[begin:end],
            table[begin:end].reshape(-1),
            query_rows,
            shares[n],
            [groups[r] for r in range(begin, end)],
            output,
        )
    return output


def solution(mesh):
    placed = (
        P(("seq", "head"), None),
        P(("seq", "head"), None),
        P(("seq", "head"), None),
        P(),
        P(),
    )

    return jax.shard_map(
        on_device, mesh=mesh, in_specs=placed, out_specs=P(("seq", "head"), None), check_vma=False
    )
```

```python
import functools
import math

import jax
import jax.numpy as jnp
from jax import lax
from jax.experimental import pallas as pl
from jax.experimental.pallas import tpu as pltpu
from jax.sharding import PartitionSpec as P


BLOCK = 128
HEAD_DIM = 128
GLOBALS = 2
RANDOM = 3
WINDOW = 3
MIB = 2**20
SOME_VMEM = 20 * MIB
MOST_VMEM = 50 * MIB


ANY = pl.BlockSpec(memory_space=pl.ANY)
SMEM = pl.BlockSpec(memory_space=pltpu.SMEM)
VMEM = pl.BlockSpec(memory_space=pltpu.VMEM)


def run_copies(copies):
    for copy in copies:
        copy.start()
    for copy in copies:
        copy.wait()


def pack_kernel(heads, order, key_ref, value_ref, *rest):
    outs, first, last = rest[:heads], rest[heads], rest[heads + 1]
    parts, edges, sem_in, sem_out, sem_edge_in, sem_edge_out = rest[heads + 2 :]
    rows = key_ref.shape[0]
    loads = []
    for r in range(heads):
        lanes = pl.ds(pl.multiple_of(order[r] * HEAD_DIM, HEAD_DIM), HEAD_DIM)
        for which, source in enumerate((key_ref, value_ref)):
            loads.append(
                pltpu.make_async_copy(
                    source.at[:, lanes], parts.at[r, which], sem_in.at[r, which]
                )
            )
    for which, source in enumerate((key_ref, value_ref)):
        for side, start in enumerate((0, rows - BLOCK)):
            loads.append(
                pltpu.make_async_copy(
                    source.at[start : start + BLOCK],
                    edges.at[side, which],
                    sem_edge_in.at[side, which],
                )
            )
    run_copies(loads)
    run_copies(
        [pltpu.make_async_copy(parts.at[r], outs[r], sem_out.at[r]) for r in range(heads)]
        + [
            pltpu.make_async_copy(edges.at[side], out, sem_edge_out.at[side])
            for side, out in enumerate((first, last))
        ]
    )


def pack(order, key_rows, value_rows):
    rows, columns = key_rows.shape
    heads = columns // HEAD_DIM
    part = jax.ShapeDtypeStruct((2, rows, HEAD_DIM), key_rows.dtype)
    edge = jax.ShapeDtypeStruct((2, BLOCK, columns), key_rows.dtype)
    return pl.pallas_call(
        functools.partial(pack_kernel, heads),
        in_specs=[SMEM, ANY, ANY],
        out_specs=[ANY] * (heads + 2),
        out_shape=[part] * heads + [edge] * 2,
        scratch_shapes=[
            pltpu.VMEM((heads, 2, rows, HEAD_DIM), key_rows.dtype),
            pltpu.VMEM((2, 2, BLOCK, columns), key_rows.dtype),
            pltpu.SemaphoreType.DMA((heads, 2)),
            pltpu.SemaphoreType.DMA((heads,)),
            pltpu.SemaphoreType.DMA((2, 2)),
            pltpu.SemaphoreType.DMA((2,)),
        ],
        compiler_params=pltpu.CompilerParams(vmem_limit_bytes=SOME_VMEM),
        name="pack",
    )(order, key_rows, value_rows)


def pick_kernel(heads, chunks, slots, order, sources, shared, *rest):
    parts, rest = rest[:heads], rest[heads:]
    outs, shared_ref, (run, sem_in, sem_out) = rest[:chunks], rest[chunks], rest[chunks + 1 :]
    rows = parts[0].shape[1]
    loads = []
    for r in range(heads):
        place = pl.ds(pl.multiple_of(order[r] * rows, BLOCK), rows)
        loads.append(pltpu.make_async_copy(parts[r], run.at[:, place], sem_in.at[r]))
    run_copies(loads)
    stores = []
    for chunk in range(chunks):
        for slot in range(slots):
            place = pl.ds(pl.multiple_of(sources[chunk * slots + slot] * BLOCK, BLOCK), BLOCK)
            stores.append(
                pltpu.make_async_copy(
                    run.at[:, place],
                    outs[chunk].at[:, slot * BLOCK : (slot + 1) * BLOCK],
                    sem_out.at[chunk, slot],
                )
            )
    for copy in stores:
        copy.start()
    for which in range(GLOBALS):
        place = pl.ds(pl.multiple_of(shared[2 * which] * BLOCK, BLOCK), BLOCK)
        block = run[:, place]
        shared_ref[:, which * BLOCK : (which + 1) * BLOCK] = jnp.where(
            shared[2 * which + 1] != 0, block, jnp.zeros_like(block)
        )
    for copy in stores:
        copy.wait()


def pick(order, sources, shared, parts, chunks, slots):
    heads = len(parts)
    rows, dtype = parts[0].shape[1], parts[0].dtype
    return pl.pallas_call(
        functools.partial(pick_kernel, heads, chunks, slots),
        in_specs=[SMEM, SMEM, SMEM] + [ANY] * heads,
        out_specs=[ANY] * chunks + [VMEM],
        out_shape=[jax.ShapeDtypeStruct((2, slots * BLOCK, HEAD_DIM), dtype)] * chunks
        + [jax.ShapeDtypeStruct((2, GLOBALS * BLOCK, HEAD_DIM), dtype)],
        scratch_shapes=[
            pltpu.VMEM((2, heads * rows, HEAD_DIM), dtype),
            pltpu.SemaphoreType.DMA((heads,)),
            pltpu.SemaphoreType.DMA((chunks, slots)),
        ],
        compiler_params=pltpu.CompilerParams(vmem_limit_bytes=SOME_VMEM),
        name="pick",
    )(order, sources, shared, *parts)


def join_kernel(count, *refs):
    sources, out_ref, sems = refs[:count], refs[count], refs[count + 1]
    copies, start = [], 0
    for place, source in enumerate(sources):
        size = source.shape[1]
        copies.append(
            pltpu.make_async_copy(source, out_ref.at[:, start : start + size], sems.at[place])
        )
        start += size
    run_copies(copies)


def join(arrays):
    rows = sum(array.shape[1] for array in arrays)
    shape = (2, rows, HEAD_DIM)
    return pl.pallas_call(
        functools.partial(join_kernel, len(arrays)),
        in_specs=[ANY] * len(arrays),
        out_specs=VMEM,
        out_shape=jax.ShapeDtypeStruct(shape, arrays[0].dtype),
        scratch_shapes=[pltpu.SemaphoreType.DMA((len(arrays),))],
        compiler_params=pltpu.CompilerParams(vmem_limit_bytes=SOME_VMEM),
        name="join",
    )(*arrays)


SCALE = math.log2(math.e) / math.sqrt(HEAD_DIM)
JOINED = 2
TOGETHER = 2


def stacked(ref, rows, head):
    return jnp.concatenate(
        [ref[rows, (head + j) * HEAD_DIM : (head + j + 1) * HEAD_DIM] for j in range(JOINED)],
        axis=0,
    )


def score_block(query, keys):
    return lax.dot_general(
        query, keys, (((1,), (1,)), ((), ())), preferred_element_type=jnp.float32
    )


def weighted(scores, top, values):
    weights = jnp.concatenate(
        [
            jnp.exp2((scores[:, start : start + HEAD_DIM] - top) * SCALE)
            for start in range(0, scores.shape[1], HEAD_DIM)
        ],
        axis=1,
    )
    both = jnp.concatenate([values, jnp.ones_like(values)], axis=1)
    mixed = jnp.dot(weights.astype(values.dtype), both, preferred_element_type=jnp.float32)
    return mixed[:, :HEAD_DIM], mixed[:, HEAD_DIM:]


def pipelined(tasks, scores_of, rest_of):
    scores = scores_of(*tasks[0])
    for place, task in enumerate(tasks):
        upcoming = scores_of(*tasks[place + 1]) if place + 1 < len(tasks) else None
        rest_of(*task, scores)
        scores = upcoming


def window_kernel(parts, order, flags, query_ref, *rest):
    locals_, (before_ref, after_ref), rest = rest[:parts], rest[parts : parts + 2], rest[parts + 2 :]
    out_ref, level_ref, held = rest
    part, step = pl.program_id(0), pl.program_id(1)
    _, width = query_ref.shape
    grouping = width // HEAD_DIM
    inner = locals_[0].shape[1]
    for r in range(parts):

        @pl.when((part == r) & (step == 0))
        def _(r=r):
            held[:, BLOCK : BLOCK + inner] = locals_[r][...]
            held[:, :BLOCK] = before_ref[...]
            held[:, BLOCK + inner :] = after_ref[...]

    def listed(which, unit):
        place = pl.ds(pl.multiple_of((step * TOGETHER + unit) * BLOCK, BLOCK), WINDOW * BLOCK)
        return held[which, place]

    def scores_of(unit, head):
        block = step * TOGETHER + unit
        scores = score_block(
            stacked(query_ref, slice(unit * BLOCK, (unit + 1) * BLOCK), head), listed(0, unit)
        )
        return jnp.concatenate(
            [
                jnp.where(flags[2 * block] != 0, scores[:, :BLOCK], -1e30),
                scores[:, BLOCK : 2 * BLOCK],
                jnp.where(flags[2 * block + 1] != 0, scores[:, 2 * BLOCK :], -1e30),
            ],
            axis=1,
        )

    def rest_of(unit, head, scores):
        top = jnp.broadcast_to(
            jnp.max(scores, axis=1, keepdims=True), (scores.shape[0], HEAD_DIM)
        )
        mixed, total = weighted(scores, top, listed(1, unit))
        mixed = mixed * (1.0 / total)
        level = top + jnp.log(total) * math.sqrt(HEAD_DIM)
        for j in range(JOINED):
            some = slice(j * BLOCK, (j + 1) * BLOCK)
            rows = slice(unit * BLOCK, (unit + 1) * BLOCK)
            lanes = slice((head + j) * HEAD_DIM, (head + j + 1) * HEAD_DIM)
            out_ref[0, rows, lanes] = mixed[some]
            level_ref[0, rows, lanes] = level[some]

    tasks = [(unit, head) for unit in range(TOGETHER) for head in range(0, grouping, JOINED)]
    pipelined(tasks, scores_of, rest_of)


def whole_block(array):
    return pl.BlockSpec(array.shape, lambda *_: (0,) * array.ndim)


def window_share(order, flags, queries, locals_, edges, begin):
    rows, columns = queries.shape
    heads = edges[0].shape[2] // HEAD_DIM
    width = columns // heads
    blocks = rows // BLOCK
    parts = len(locals_)
    pairs = parts * blocks * (width // HEAD_DIM) * BLOCK * WINDOW * BLOCK
    some = TOGETHER * BLOCK
    edge = pl.BlockSpec((2, BLOCK, HEAD_DIM), lambda r, i, order, flags: (0, 0, order[begin + r]))
    return pl.pallas_call(
        functools.partial(window_kernel, parts),
        grid_spec=pltpu.PrefetchScalarGridSpec(
            num_scalar_prefetch=2,
            grid=(parts, blocks // TOGETHER),
            in_specs=[pl.BlockSpec((some, width), lambda r, i, order, flags: (i, order[begin + r]))]
            + [whole_block(array) for array in locals_]
            + [edge, edge],
            out_specs=[pl.BlockSpec((1, some, width), lambda r, i, order, flags: (r, i, 0))] * 2,
            scratch_shapes=[pltpu.VMEM((2, rows + 2 * BLOCK, HEAD_DIM), queries.dtype)],
        ),
        out_shape=[jax.ShapeDtypeStruct((parts, rows, width), jnp.float32)] * 2,
        compiler_params=pltpu.CompilerParams(vmem_limit_bytes=MOST_VMEM),
        cost_estimate=pl.CostEstimate(
            flops=4 * pairs * HEAD_DIM, bytes_accessed=8 * MIB, transcendentals=pairs
        ),
        name="window",
    )(order, flags, queries, *locals_, *edges)


LISTED = GLOBALS + RANDOM


def finish_kernel(begin, counts, aliased, order, table, query_ref, mixed_ref, level_ref, *rest):
    sources, (out_ref, held) = rest[: sum(counts)], rest[sum(counts) + aliased :]
    part, step = pl.program_id(0), pl.program_id(1)
    grouping = query_ref.shape[1] // HEAD_DIM
    number = 0
    for r, count in enumerate(counts):

        @pl.when((part == r) & (step == 0))
        def _(mine=sources[number : number + count]):
            start = 0
            for source in mine:
                held[:, start : start + source.shape[1]] = source[...]
                start += source.shape[1]

        number += count
    base = ((begin + part) * pl.num_programs(1) + step) * TOGETHER * LISTED

    def listed(which, unit):
        return jnp.concatenate(
            [
                held[
                    which,
                    pl.ds(pl.multiple_of(table[base + unit * LISTED + n] * BLOCK, BLOCK), BLOCK),
                ]
                for n in range(LISTED)
            ],
            axis=0,
        )

    def scores_of(unit, head):
        return score_block(
            stacked(query_ref, slice(unit * BLOCK, (unit + 1) * BLOCK), head), listed(0, unit)
        )

    def rest_of(unit, head, scores):
        rows = slice(unit * BLOCK, (unit + 1) * BLOCK)
        level = stacked(level_ref.at[0], rows, head)
        top = jnp.maximum(level, jnp.max(scores, axis=1, keepdims=True))
        mixed, total = weighted(scores, top, listed(1, unit))
        kept = jnp.exp2((level - top) * SCALE)
        inverse = 1.0 / (total + kept)
        mixed = (mixed + stacked(mixed_ref.at[0], rows, head) * kept) * inverse
        for j in range(JOINED):
            lanes = slice((head + j) * HEAD_DIM, (head + j + 1) * HEAD_DIM)
            out_ref[rows, lanes] = mixed[j * BLOCK : (j + 1) * BLOCK].astype(out_ref.dtype)

    tasks = [(unit, head) for unit in range(TOGETHER) for head in range(0, grouping, JOINED)]
    pipelined(tasks, scores_of, rest_of)


def finish(order, table, queries, share, parts, begin, output):
    rows, columns = queries.shape
    width = share[0].shape[2]
    blocks = rows // BLOCK
    arrays = [array for part in parts for array in part]
    pairs = len(parts) * blocks * (width // HEAD_DIM) * BLOCK * LISTED * BLOCK
    some = TOGETHER * BLOCK
    spec = pl.BlockSpec((some, width), lambda r, i, order, table: (i, order[begin + r]))
    aliased = [] if output is None else [output]
    operands = (order, table, queries, *share, *arrays, *aliased)
    return pl.pallas_call(
        functools.partial(finish_kernel, begin, [len(part) for part in parts], len(aliased)),
        grid_spec=pltpu.PrefetchScalarGridSpec(
            num_scalar_prefetch=2,
            grid=(len(parts), blocks // TOGETHER),
            in_specs=[
                spec,
            ]
            + [pl.BlockSpec((1, some, width), lambda r, i, order, table: (r, i, 0))] * 2
            + [whole_block(array) for array in arrays]
            + [ANY] * len(aliased),
            out_specs=spec,
            scratch_shapes=[
                pltpu.VMEM(
                    (2, sum(array.shape[1] for array in parts[0]), HEAD_DIM), queries.dtype
                ),
            ],
        ),
        out_shape=jax.ShapeDtypeStruct((rows, columns), queries.dtype),
        input_output_aliases={len(operands) - 1: 0} if aliased else {},
        compiler_params=pltpu.CompilerParams(vmem_limit_bytes=MOST_VMEM),
        cost_estimate=pl.CostEstimate(
            flops=4 * pairs * HEAD_DIM, bytes_accessed=8 * MIB, transcendentals=pairs
        ),
        name="finish",
    )(*operands)


def plan(random_table, seq_index, head_index, seq_count, heads, my_blocks, slots):
    blocks = random_table.shape[0]
    run_blocks = blocks // seq_count
    by_run = random_table.reshape(seq_count, run_blocks, heads, RANDOM)
    mine = lax.dynamic_index_in_dim(by_run, head_index, 2, keepdims=False)
    mine = mine.reshape(seq_count, run_blocks * RANDOM) - seq_index * run_blocks
    local = jnp.arange(run_blocks, dtype=jnp.int32)
    named = jnp.any(mine[:, None, :] == local[:, None], axis=2)
    rank = jnp.sum(named[:, None, :] & (local[None, :] < local[:, None]), axis=2)
    hit = named[:, None, :] & (rank[:, None, :] == jnp.arange(slots)[:, None])
    sources = jnp.sum(jnp.where(hit, local, 0), axis=2).astype(jnp.int32)
    run = lax.dynamic_index_in_dim(by_run, seq_index, 0, keepdims=False)
    run = run.transpose(1, 0, 2).reshape(heads, run_blocks * RANDOM)
    order_of = jnp.arange(run_blocks * RANDOM)
    earlier = order_of[None, :] < order_of[:, None]
    first = ~jnp.any((run[:, :, None] == run[:, None, :]) & earlier, axis=2)
    start = head_index * my_blocks * RANDOM
    wanted = lax.dynamic_slice_in_dim(run, start, my_blocks * RANDOM, 1)
    same = (wanted[:, :, None] // run_blocks) == (run[:, None, :] // run_blocks)
    below = run[:, None, :] < wanted[:, :, None]
    slot = jnp.sum(same & below & first[:, None, :], axis=2).astype(jnp.int32)
    return sources, wanted // run_blocks, slot


def on_device(query_rows, key_rows, value_rows, random_table, global_blocks):
    seq_count, heads = lax.axis_size("seq"), lax.axis_size("head")
    seq_index, head_index = lax.axis_index("seq"), lax.axis_index("head")
    rows = key_rows.shape[0]
    my_blocks = rows // BLOCK
    run_blocks = my_blocks * heads
    slots = max(1, (RANDOM * run_blocks + 2 * seq_count - 1) // (2 * seq_count))
    order = head_index ^ jnp.arange(heads, dtype=jnp.int32)
    chunk_of = seq_index ^ jnp.arange(seq_count, dtype=jnp.int32)

    def across(array, axis, bit):
        count = lax.axis_size(axis)
        return lax.ppermute(array, axis, [(i, i ^ bit) for i in range(count)])

    *parts, first, last = pack(order, key_rows, value_rows)
    arrived = [parts[0]] + [across(parts[r], "head", r) for r in range(heads - 1, 0, -1)][::-1]

    flat = seq_count * heads
    previous = lax.ppermute(last, ("seq", "head"), [(i, i + 1) for i in range(flat - 1)])
    upcoming = lax.ppermute(first, ("seq", "head"), [(i + 1, i) for i in range(flat - 1)])

    sources, owner, slot = plan(
        random_table, seq_index, head_index, seq_count, heads, my_blocks, slots
    )
    sources = jnp.take(sources, chunk_of, axis=0).reshape(-1)
    shared = jnp.stack(
        [global_blocks % run_blocks, (global_blocks // run_blocks == seq_index).astype(jnp.int32)],
        axis=1,
    ).reshape(-1)
    picked = pick(order, sources, shared, arrived, seq_count, slots)
    outgoing, common = picked[:seq_count], picked[seq_count]
    chunks = [outgoing[0]] + [across(outgoing[k], "seq", k) for k in range(1, seq_count)]
    bit = seq_count // 2
    while bit:
        common = common + across(common, "seq", bit)
        bit //= 2
    half, last_part = seq_count // 2, (seq_count + seq_count // 2) // 2
    own = [
        chunks[0],
        join(chunks[1:half]),
        join([common] + chunks[half:last_part]),
        join(chunks[last_part:]),
    ]
    groups = {0: own}
    bit = heads // 2
    while bit:
        for r in sorted(groups):
            groups[r + bit] = [across(array, "head", bit) for array in groups[r]]
        bit //= 2

    local = jnp.arange(my_blocks, dtype=jnp.int32)
    chunk = owner ^ seq_index
    place = chunk * slots + slot + jnp.where(chunk >= half, GLOBALS, 0)
    place = jnp.take(place, order, axis=0).reshape(heads, my_blocks, RANDOM)
    commons = half * slots + jnp.arange(GLOBALS, dtype=jnp.int32)
    commons = jnp.broadcast_to(commons, (heads, my_blocks, GLOBALS))
    table = jnp.concatenate([commons, place], axis=2).reshape(-1)
    number = (seq_index * heads + head_index) * my_blocks + local
    flags = (
        jnp.stack([number > 0, number < seq_count * run_blocks - 1], axis=1)
        .astype(jnp.int32)
        .reshape(-1)
    )
    half_heads = heads // 2
    shares = []
    for some in (slice(0, half_heads), slice(half_heads, heads)):
        shares.append(
            window_share(order, flags, query_rows, parts[some], (previous, upcoming), some.start)
        )
    output = None
    for n, (begin, end) in enumerate(((0, half_heads), (half_heads, heads))):
        output = finish(
            order,
            table,
            query_rows,
            shares[n],
            [groups[r] for r in range(begin, end)],
            begin,
            output,
        )
    return output


def solution(mesh):
    placed = (
        P(("seq", "head"), None),
        P(("seq", "head"), None),
        P(("seq", "head"), None),
        P(),
        P(),
    )

    return jax.shard_map(
        on_device, mesh=mesh, in_specs=placed, out_specs=P(("seq", "head"), None), check_vma=False
    )
```

```python
import functools
import math

import jax
import jax.numpy as jnp
from jax import lax
from jax.experimental import pallas as pl
from jax.experimental.pallas import tpu as pltpu
from jax.sharding import PartitionSpec as P


BLOCK = 128
HEAD_DIM = 128
GLOBALS = 2
RANDOM = 3
WINDOW = 3
MIB = 2**20
SOME_VMEM = 20 * MIB
MOST_VMEM = 60 * MIB
LESS_VMEM = 50 * MIB


ANY = pl.BlockSpec(memory_space=pl.ANY)
SMEM = pl.BlockSpec(memory_space=pltpu.SMEM)
VMEM = pl.BlockSpec(memory_space=pltpu.VMEM)


def run_copies(copies):
    for copy in copies:
        copy.start()
    for copy in copies:
        copy.wait()


def pack_kernel(heads, order, key_ref, value_ref, *rest):
    outs, first, last = rest[:heads], rest[heads], rest[heads + 1]
    parts, edges, sem_in, sem_out, sem_edge_in, sem_edge_out = rest[heads + 2 :]
    rows = key_ref.shape[0]
    loads = []
    for r in range(heads):
        lanes = pl.ds(pl.multiple_of(order[r] * HEAD_DIM, HEAD_DIM), HEAD_DIM)
        for which, source in enumerate((key_ref, value_ref)):
            loads.append(
                pltpu.make_async_copy(
                    source.at[:, lanes], parts.at[r, which], sem_in.at[r, which]
                )
            )
    for which, source in enumerate((key_ref, value_ref)):
        for side, start in enumerate((0, rows - BLOCK)):
            loads.append(
                pltpu.make_async_copy(
                    source.at[start : start + BLOCK],
                    edges.at[side, which],
                    sem_edge_in.at[side, which],
                )
            )
    run_copies(loads)
    run_copies(
        [pltpu.make_async_copy(parts.at[r], outs[r], sem_out.at[r]) for r in range(heads)]
        + [
            pltpu.make_async_copy(edges.at[side], out, sem_edge_out.at[side])
            for side, out in enumerate((first, last))
        ]
    )


def pack(order, key_rows, value_rows):
    rows, columns = key_rows.shape
    heads = columns // HEAD_DIM
    part = jax.ShapeDtypeStruct((2, rows, HEAD_DIM), key_rows.dtype)
    edge = jax.ShapeDtypeStruct((2, BLOCK, columns), key_rows.dtype)
    return pl.pallas_call(
        functools.partial(pack_kernel, heads),
        in_specs=[SMEM, ANY, ANY],
        out_specs=[ANY] * (heads + 2),
        out_shape=[part] * heads + [edge] * 2,
        scratch_shapes=[
            pltpu.VMEM((heads, 2, rows, HEAD_DIM), key_rows.dtype),
            pltpu.VMEM((2, 2, BLOCK, columns), key_rows.dtype),
            pltpu.SemaphoreType.DMA((heads, 2)),
            pltpu.SemaphoreType.DMA((heads,)),
            pltpu.SemaphoreType.DMA((2, 2)),
            pltpu.SemaphoreType.DMA((2,)),
        ],
        compiler_params=pltpu.CompilerParams(vmem_limit_bytes=SOME_VMEM),
        name="pack",
    )(order, key_rows, value_rows)


def pick_kernel(heads, chunks, slots, order, sources, shared, *rest):
    parts, rest = rest[:heads], rest[heads:]
    outs, shared_ref, (run, sem_in, sem_out) = rest[:chunks], rest[chunks], rest[chunks + 1 :]
    rows = parts[0].shape[1]
    loads = []
    for r in range(heads):
        place = pl.ds(pl.multiple_of(order[r] * rows, BLOCK), rows)
        loads.append(pltpu.make_async_copy(parts[r], run.at[:, place], sem_in.at[r]))
    run_copies(loads)
    stores = []
    for chunk in range(chunks):
        for slot in range(slots):
            place = pl.ds(pl.multiple_of(sources[chunk * slots + slot] * BLOCK, BLOCK), BLOCK)
            stores.append(
                pltpu.make_async_copy(
                    run.at[:, place],
                    outs[chunk].at[:, slot * BLOCK : (slot + 1) * BLOCK],
                    sem_out.at[chunk, slot],
                )
            )
    for copy in stores:
        copy.start()
    for which in range(GLOBALS):
        place = pl.ds(pl.multiple_of(shared[2 * which] * BLOCK, BLOCK), BLOCK)
        block = run[:, place]
        shared_ref[:, which * BLOCK : (which + 1) * BLOCK] = jnp.where(
            shared[2 * which + 1] != 0, block, jnp.zeros_like(block)
        )
    for copy in stores:
        copy.wait()


def pick(order, sources, shared, parts, chunks, slots):
    heads = len(parts)
    rows, dtype = parts[0].shape[1], parts[0].dtype
    return pl.pallas_call(
        functools.partial(pick_kernel, heads, chunks, slots),
        in_specs=[SMEM, SMEM, SMEM] + [ANY] * heads,
        out_specs=[ANY] * chunks + [VMEM],
        out_shape=[jax.ShapeDtypeStruct((2, slots * BLOCK, HEAD_DIM), dtype)] * chunks
        + [jax.ShapeDtypeStruct((2, GLOBALS * BLOCK, HEAD_DIM), dtype)],
        scratch_shapes=[
            pltpu.VMEM((2, heads * rows, HEAD_DIM), dtype),
            pltpu.SemaphoreType.DMA((heads,)),
            pltpu.SemaphoreType.DMA((chunks, slots)),
        ],
        compiler_params=pltpu.CompilerParams(vmem_limit_bytes=SOME_VMEM),
        name="pick",
    )(order, sources, shared, *parts)


def join_kernel(count, *refs):
    sources, out_ref, sems = refs[:count], refs[count], refs[count + 1]
    copies, start = [], 0
    for place, source in enumerate(sources):
        size = source.shape[1]
        copies.append(
            pltpu.make_async_copy(source, out_ref.at[:, start : start + size], sems.at[place])
        )
        start += size
    run_copies(copies)


def join(arrays):
    rows = sum(array.shape[1] for array in arrays)
    shape = (2, rows, HEAD_DIM)
    return pl.pallas_call(
        functools.partial(join_kernel, len(arrays)),
        in_specs=[ANY] * len(arrays),
        out_specs=VMEM,
        out_shape=jax.ShapeDtypeStruct(shape, arrays[0].dtype),
        scratch_shapes=[pltpu.SemaphoreType.DMA((len(arrays),))],
        compiler_params=pltpu.CompilerParams(vmem_limit_bytes=SOME_VMEM),
        name="join",
    )(*arrays)


SCALE = math.log2(math.e) / math.sqrt(HEAD_DIM)
JOINED = 2
TOGETHER = 2


def stacked(ref, rows, head):
    return jnp.concatenate(
        [ref[rows, (head + j) * HEAD_DIM : (head + j + 1) * HEAD_DIM] for j in range(JOINED)],
        axis=0,
    )


def score_block(query, keys):
    return lax.dot_general(
        query, keys, (((1,), (1,)), ((), ())), preferred_element_type=jnp.float32
    )


def weighted(scores, top, values):
    weights = jnp.concatenate(
        [
            jnp.exp2((scores[:, start : start + HEAD_DIM] - top) * SCALE)
            for start in range(0, scores.shape[1], HEAD_DIM)
        ],
        axis=1,
    )
    both = jnp.concatenate([values, jnp.ones_like(values)], axis=1)
    mixed = jnp.dot(weights.astype(values.dtype), both, preferred_element_type=jnp.float32)
    return mixed[:, :HEAD_DIM], mixed[:, HEAD_DIM:]


def pipelined(tasks, scores_of, rest_of):
    scores = scores_of(*tasks[0])
    for place, task in enumerate(tasks):
        upcoming = scores_of(*tasks[place + 1]) if place + 1 < len(tasks) else None
        rest_of(*task, scores)
        scores = upcoming


def window_kernel(parts, order, flags, query_ref, *rest):
    locals_, (before_ref, after_ref), rest = rest[:parts], rest[parts : parts + 2], rest[parts + 2 :]
    out_ref, level_ref, held = rest
    part, step = pl.program_id(0), pl.program_id(1)
    _, width = query_ref.shape
    grouping = width // HEAD_DIM
    inner = locals_[0].shape[1]
    for r in range(parts):

        @pl.when((part == r) & (step == 0))
        def _(r=r):
            held[:, BLOCK : BLOCK + inner] = locals_[r][...]
            held[:, :BLOCK] = before_ref[...]
            held[:, BLOCK + inner :] = after_ref[...]

    def listed(which, unit):
        place = pl.ds(pl.multiple_of((step * TOGETHER + unit) * BLOCK, BLOCK), WINDOW * BLOCK)
        return held[which, place]

    def scores_of(unit, head):
        block = step * TOGETHER + unit
        scores = score_block(
            stacked(query_ref, slice(unit * BLOCK, (unit + 1) * BLOCK), head), listed(0, unit)
        )
        return jnp.concatenate(
            [
                jnp.where(flags[2 * block] != 0, scores[:, :BLOCK], -1e30),
                scores[:, BLOCK : 2 * BLOCK],
                jnp.where(flags[2 * block + 1] != 0, scores[:, 2 * BLOCK :], -1e30),
            ],
            axis=1,
        )

    def rest_of(unit, head, scores):
        top = jnp.broadcast_to(
            jnp.max(scores, axis=1, keepdims=True), (scores.shape[0], HEAD_DIM)
        )
        mixed, total = weighted(scores, top, listed(1, unit))
        mixed = mixed * (1.0 / total)
        level = top + jnp.log(total) * math.sqrt(HEAD_DIM)
        for j in range(JOINED):
            some = slice(j * BLOCK, (j + 1) * BLOCK)
            rows = slice(unit * BLOCK, (unit + 1) * BLOCK)
            lanes = slice((head + j) * HEAD_DIM, (head + j + 1) * HEAD_DIM)
            out_ref[0, rows, lanes] = mixed[some]
            level_ref[0, rows, lanes] = level[some]

    tasks = [(unit, head) for unit in range(TOGETHER) for head in range(0, grouping, JOINED)]
    pipelined(tasks, scores_of, rest_of)


def whole_block(array):
    return pl.BlockSpec(array.shape, lambda *_: (0,) * array.ndim)


def window_share(order, flags, queries, locals_, edges, begin):
    rows, columns = queries.shape
    heads = edges[0].shape[2] // HEAD_DIM
    width = columns // heads
    blocks = rows // BLOCK
    parts = len(locals_)
    pairs = parts * blocks * (width // HEAD_DIM) * BLOCK * WINDOW * BLOCK
    some = TOGETHER * BLOCK
    edge = pl.BlockSpec((2, BLOCK, HEAD_DIM), lambda r, i, order, flags: (0, 0, order[begin + r]))
    return pl.pallas_call(
        functools.partial(window_kernel, parts),
        grid_spec=pltpu.PrefetchScalarGridSpec(
            num_scalar_prefetch=2,
            grid=(parts, blocks // TOGETHER),
            in_specs=[pl.BlockSpec((some, width), lambda r, i, order, flags: (i, order[begin + r]))]
            + [whole_block(array) for array in locals_]
            + [edge, edge],
            out_specs=[pl.BlockSpec((1, some, width), lambda r, i, order, flags: (r, i, 0))] * 2,
            scratch_shapes=[pltpu.VMEM((2, rows + 2 * BLOCK, HEAD_DIM), queries.dtype)],
        ),
        out_shape=[jax.ShapeDtypeStruct((parts, rows, width), jnp.float32)] * 2,
        compiler_params=pltpu.CompilerParams(vmem_limit_bytes=LESS_VMEM if begin == 0 else MOST_VMEM),
        cost_estimate=pl.CostEstimate(
            flops=4 * pairs * HEAD_DIM, bytes_accessed=8 * MIB, transcendentals=pairs
        ),
        name="window",
    )(order, flags, queries, *locals_, *edges)


LISTED = GLOBALS + RANDOM


def finish_kernel(begin, counts, aliased, order, table, query_ref, mixed_ref, level_ref, *rest):
    sources, (out_ref, held) = rest[: sum(counts)], rest[sum(counts) + aliased :]
    part, step = pl.program_id(0), pl.program_id(1)
    grouping = query_ref.shape[1] // HEAD_DIM
    number = 0
    for r, count in enumerate(counts):

        @pl.when((part == r) & (step == 0))
        def _(mine=sources[number : number + count]):
            start = 0
            for source in mine:
                held[:, start : start + source.shape[1]] = source[...]
                start += source.shape[1]

        number += count
    base = ((begin + part) * pl.num_programs(1) + step) * TOGETHER * LISTED

    def listed(which, unit):
        return jnp.concatenate(
            [
                held[
                    which,
                    pl.ds(pl.multiple_of(table[base + unit * LISTED + n] * BLOCK, BLOCK), BLOCK),
                ]
                for n in range(LISTED)
            ],
            axis=0,
        )

    def scores_of(unit, head):
        return score_block(
            stacked(query_ref, slice(unit * BLOCK, (unit + 1) * BLOCK), head), listed(0, unit)
        )

    def rest_of(unit, head, scores):
        rows = slice(unit * BLOCK, (unit + 1) * BLOCK)
        level = stacked(level_ref.at[0], rows, head)
        top = jnp.maximum(level, jnp.max(scores, axis=1, keepdims=True))
        mixed, total = weighted(scores, top, listed(1, unit))
        kept = jnp.exp2((level - top) * SCALE)
        inverse = 1.0 / (total + kept)
        mixed = (mixed + stacked(mixed_ref.at[0], rows, head) * kept) * inverse
        for j in range(JOINED):
            lanes = slice((head + j) * HEAD_DIM, (head + j + 1) * HEAD_DIM)
            out_ref[rows, lanes] = mixed[j * BLOCK : (j + 1) * BLOCK].astype(out_ref.dtype)

    tasks = [(unit, head) for unit in range(TOGETHER) for head in range(0, grouping, JOINED)]
    pipelined(tasks, scores_of, rest_of)


def finish(order, table, queries, share, parts, begin, output):
    rows, columns = queries.shape
    width = share[0].shape[2]
    blocks = rows // BLOCK
    arrays = [array for part in parts for array in part]
    pairs = len(parts) * blocks * (width // HEAD_DIM) * BLOCK * LISTED * BLOCK
    some = TOGETHER * BLOCK
    spec = pl.BlockSpec((some, width), lambda r, i, order, table: (i, order[begin + r]))
    aliased = [] if output is None else [output]
    operands = (order, table, queries, *share, *arrays, *aliased)
    return pl.pallas_call(
        functools.partial(finish_kernel, begin, [len(part) for part in parts], len(aliased)),
        grid_spec=pltpu.PrefetchScalarGridSpec(
            num_scalar_prefetch=2,
            grid=(len(parts), blocks // TOGETHER),
            in_specs=[
                spec,
            ]
            + [pl.BlockSpec((1, some, width), lambda r, i, order, table: (r, i, 0))] * 2
            + [whole_block(array) for array in arrays]
            + [ANY] * len(aliased),
            out_specs=spec,
            scratch_shapes=[
                pltpu.VMEM(
                    (2, sum(array.shape[1] for array in parts[0]), HEAD_DIM), queries.dtype
                ),
            ],
        ),
        out_shape=jax.ShapeDtypeStruct((rows, columns), queries.dtype),
        input_output_aliases={len(operands) - 1: 0} if aliased else {},
        compiler_params=pltpu.CompilerParams(vmem_limit_bytes=LESS_VMEM),
        cost_estimate=pl.CostEstimate(
            flops=4 * pairs * HEAD_DIM, bytes_accessed=8 * MIB, transcendentals=pairs
        ),
        name="finish",
    )(*operands)


def plan(random_table, seq_index, head_index, seq_count, heads, my_blocks, slots):
    blocks = random_table.shape[0]
    run_blocks = blocks // seq_count
    by_run = random_table.reshape(seq_count, run_blocks, heads, RANDOM)
    mine = lax.dynamic_index_in_dim(by_run, head_index, 2, keepdims=False)
    mine = mine.reshape(seq_count, run_blocks * RANDOM) - seq_index * run_blocks
    local = jnp.arange(run_blocks, dtype=jnp.int32)
    named = jnp.any(mine[:, None, :] == local[:, None], axis=2)
    rank = jnp.sum(named[:, None, :] & (local[None, :] < local[:, None]), axis=2)
    hit = named[:, None, :] & (rank[:, None, :] == jnp.arange(slots)[:, None])
    sources = jnp.sum(jnp.where(hit, local, 0), axis=2).astype(jnp.int32)
    run = lax.dynamic_index_in_dim(by_run, seq_index, 0, keepdims=False)
    run = run.transpose(1, 0, 2).reshape(heads, run_blocks * RANDOM)
    order_of = jnp.arange(run_blocks * RANDOM)
    earlier = order_of[None, :] < order_of[:, None]
    first = ~jnp.any((run[:, :, None] == run[:, None, :]) & earlier, axis=2)
    start = head_index * my_blocks * RANDOM
    wanted = lax.dynamic_slice_in_dim(run, start, my_blocks * RANDOM, 1)
    same = (wanted[:, :, None] // run_blocks) == (run[:, None, :] // run_blocks)
    below = run[:, None, :] < wanted[:, :, None]
    slot = jnp.sum(same & below & first[:, None, :], axis=2).astype(jnp.int32)
    return sources, wanted // run_blocks, slot


def on_device(query_rows, key_rows, value_rows, random_table, global_blocks):
    seq_count, heads = lax.axis_size("seq"), lax.axis_size("head")
    seq_index, head_index = lax.axis_index("seq"), lax.axis_index("head")
    rows = key_rows.shape[0]
    my_blocks = rows // BLOCK
    run_blocks = my_blocks * heads
    slots = max(1, (RANDOM * run_blocks + 2 * seq_count - 1) // (2 * seq_count))
    order = head_index ^ jnp.arange(heads, dtype=jnp.int32)
    chunk_of = seq_index ^ jnp.arange(seq_count, dtype=jnp.int32)

    def across(array, axis, bit):
        count = lax.axis_size(axis)
        return lax.ppermute(array, axis, [(i, i ^ bit) for i in range(count)])

    *parts, first, last = pack(order, key_rows, value_rows)
    arrived = [parts[0]] + [across(parts[r], "head", r) for r in range(heads - 1, 0, -1)][::-1]

    flat = seq_count * heads
    previous = lax.ppermute(last, ("seq", "head"), [(i, i + 1) for i in range(flat - 1)])
    upcoming = lax.ppermute(first, ("seq", "head"), [(i + 1, i) for i in range(flat - 1)])

    sources, owner, slot = plan(
        random_table, seq_index, head_index, seq_count, heads, my_blocks, slots
    )
    sources = jnp.take(sources, chunk_of, axis=0).reshape(-1)
    shared = jnp.stack(
        [global_blocks % run_blocks, (global_blocks // run_blocks == seq_index).astype(jnp.int32)],
        axis=1,
    ).reshape(-1)
    picked = pick(order, sources, shared, arrived, seq_count, slots)
    outgoing, common = picked[:seq_count], picked[seq_count]
    chunks = [outgoing[0]] + [across(outgoing[k], "seq", k) for k in range(1, seq_count)]
    bit = seq_count // 2
    while bit:
        common = common + across(common, "seq", bit)
        bit //= 2
    half, last_part = seq_count // 2, (seq_count + seq_count // 2) // 2
    own = [join(chunks[:half]), join(chunks[half:last_part]), join(chunks[last_part:] + [common])]
    groups = {0: own}
    bit = heads // 2
    while bit:
        for r in sorted(groups):
            groups[r + bit] = [across(array, "head", bit) for array in groups[r]]
        bit //= 2

    local = jnp.arange(my_blocks, dtype=jnp.int32)
    chunk = owner ^ seq_index
    place = chunk * slots + slot
    place = jnp.take(place, order, axis=0).reshape(heads, my_blocks, RANDOM)
    commons = seq_count * slots + jnp.arange(GLOBALS, dtype=jnp.int32)
    commons = jnp.broadcast_to(commons, (heads, my_blocks, GLOBALS))
    table = jnp.concatenate([commons, place], axis=2).reshape(-1)
    number = (seq_index * heads + head_index) * my_blocks + local
    flags = (
        jnp.stack([number > 0, number < seq_count * run_blocks - 1], axis=1)
        .astype(jnp.int32)
        .reshape(-1)
    )
    half_heads = heads // 2
    shares = []
    for some in (slice(0, half_heads), slice(half_heads, heads)):
        shares.append(
            window_share(order, flags, query_rows, parts[some], (previous, upcoming), some.start)
        )
    output = None
    for n, (begin, end) in enumerate(((0, half_heads), (half_heads, heads))):
        output = finish(
            order,
            table,
            query_rows,
            shares[n],
            [groups[r] for r in range(begin, end)],
            begin,
            output,
        )
    return output


def solution(mesh):
    placed = (
        P(("seq", "head"), None),
        P(("seq", "head"), None),
        P(("seq", "head"), None),
        P(),
        P(),
    )

    return jax.shard_map(
        on_device, mesh=mesh, in_specs=placed, out_specs=P(("seq", "head"), None), check_vma=False
    )
```

```python
import functools
import math

import jax
import jax.numpy as jnp
from jax import lax
from jax.experimental import pallas as pl
from jax.experimental.pallas import tpu as pltpu
from jax.sharding import PartitionSpec as P


BLOCK = 128
HEAD_DIM = 128
GLOBALS = 2
RANDOM = 3
WINDOW = 3
MIB = 2**20
SOME_VMEM = 20 * MIB
MOST_VMEM = 60 * MIB
LESS_VMEM = 50 * MIB


ANY = pl.BlockSpec(memory_space=pl.ANY)
SMEM = pl.BlockSpec(memory_space=pltpu.SMEM)
VMEM = pl.BlockSpec(memory_space=pltpu.VMEM)


def run_copies(copies):
    for copy in copies:
        copy.start()
    for copy in copies:
        copy.wait()


def pack_kernel(heads, order, key_ref, value_ref, *rest):
    outs, first, last = rest[:heads], rest[heads], rest[heads + 1]
    parts, edges, sem_in, sem_out, sem_edge_in, sem_edge_out = rest[heads + 2 :]
    rows = key_ref.shape[0]
    loads = []
    for r in range(heads):
        lanes = pl.ds(pl.multiple_of(order[r] * HEAD_DIM, HEAD_DIM), HEAD_DIM)
        for which, source in enumerate((key_ref, value_ref)):
            loads.append(
                pltpu.make_async_copy(
                    source.at[:, lanes], parts.at[r, which], sem_in.at[r, which]
                )
            )
    for which, source in enumerate((key_ref, value_ref)):
        for side, start in enumerate((0, rows - BLOCK)):
            loads.append(
                pltpu.make_async_copy(
                    source.at[start : start + BLOCK],
                    edges.at[side, which],
                    sem_edge_in.at[side, which],
                )
            )
    run_copies(loads)
    run_copies(
        [pltpu.make_async_copy(parts.at[r], outs[r], sem_out.at[r]) for r in range(heads)]
        + [
            pltpu.make_async_copy(edges.at[side], out, sem_edge_out.at[side])
            for side, out in enumerate((first, last))
        ]
    )


def pack(order, key_rows, value_rows):
    rows, columns = key_rows.shape
    heads = columns // HEAD_DIM
    part = jax.ShapeDtypeStruct((2, rows, HEAD_DIM), key_rows.dtype)
    edge = jax.ShapeDtypeStruct((2, BLOCK, columns), key_rows.dtype)
    return pl.pallas_call(
        functools.partial(pack_kernel, heads),
        in_specs=[SMEM, ANY, ANY],
        out_specs=[ANY] * (heads + 2),
        out_shape=[part] * heads + [edge] * 2,
        scratch_shapes=[
            pltpu.VMEM((heads, 2, rows, HEAD_DIM), key_rows.dtype),
            pltpu.VMEM((2, 2, BLOCK, columns), key_rows.dtype),
            pltpu.SemaphoreType.DMA((heads, 2)),
            pltpu.SemaphoreType.DMA((heads,)),
            pltpu.SemaphoreType.DMA((2, 2)),
            pltpu.SemaphoreType.DMA((2,)),
        ],
        compiler_params=pltpu.CompilerParams(vmem_limit_bytes=SOME_VMEM),
        name="pack",
    )(order, key_rows, value_rows)


def pick_kernel(heads, chunks, slots, order, sources, shared, *rest):
    parts, rest = rest[:heads], rest[heads:]
    outs, shared_ref, (run, sem_in, sem_out) = rest[:chunks], rest[chunks], rest[chunks + 1 :]
    rows = parts[0].shape[1]
    loads = []
    for r in range(heads):
        place = pl.ds(pl.multiple_of(order[r] * rows, BLOCK), rows)
        loads.append(pltpu.make_async_copy(parts[r], run.at[:, place], sem_in.at[r]))
    run_copies(loads)
    stores = []
    for chunk in range(chunks):
        for slot in range(slots):
            place = pl.ds(pl.multiple_of(sources[chunk * slots + slot] * BLOCK, BLOCK), BLOCK)
            stores.append(
                pltpu.make_async_copy(
                    run.at[:, place],
                    outs[chunk].at[:, slot * BLOCK : (slot + 1) * BLOCK],
                    sem_out.at[chunk, slot],
                )
            )
    for copy in stores:
        copy.start()
    for which in range(GLOBALS):
        place = pl.ds(pl.multiple_of(shared[2 * which] * BLOCK, BLOCK), BLOCK)
        block = run[:, place]
        shared_ref[:, which * BLOCK : (which + 1) * BLOCK] = jnp.where(
            shared[2 * which + 1] != 0, block, jnp.zeros_like(block)
        )
    for copy in stores:
        copy.wait()


def pick(order, sources, shared, parts, chunks, slots):
    heads = len(parts)
    rows, dtype = parts[0].shape[1], parts[0].dtype
    return pl.pallas_call(
        functools.partial(pick_kernel, heads, chunks, slots),
        in_specs=[SMEM, SMEM, SMEM] + [ANY] * heads,
        out_specs=[ANY] * chunks + [VMEM],
        out_shape=[jax.ShapeDtypeStruct((2, slots * BLOCK, HEAD_DIM), dtype)] * chunks
        + [jax.ShapeDtypeStruct((2, GLOBALS * BLOCK, HEAD_DIM), dtype)],
        scratch_shapes=[
            pltpu.VMEM((2, heads * rows, HEAD_DIM), dtype),
            pltpu.SemaphoreType.DMA((heads,)),
            pltpu.SemaphoreType.DMA((chunks, slots)),
        ],
        compiler_params=pltpu.CompilerParams(vmem_limit_bytes=SOME_VMEM),
        name="pick",
    )(order, sources, shared, *parts)


def join_kernel(count, *refs):
    sources, out_ref, sems = refs[:count], refs[count], refs[count + 1]
    copies, start = [], 0
    for place, source in enumerate(sources):
        size = source.shape[1]
        copies.append(
            pltpu.make_async_copy(source, out_ref.at[:, start : start + size], sems.at[place])
        )
        start += size
    run_copies(copies)


def join(arrays):
    rows = sum(array.shape[1] for array in arrays)
    shape = (2, rows, HEAD_DIM)
    return pl.pallas_call(
        functools.partial(join_kernel, len(arrays)),
        in_specs=[ANY] * len(arrays),
        out_specs=VMEM,
        out_shape=jax.ShapeDtypeStruct(shape, arrays[0].dtype),
        scratch_shapes=[pltpu.SemaphoreType.DMA((len(arrays),))],
        compiler_params=pltpu.CompilerParams(vmem_limit_bytes=SOME_VMEM),
        name="join",
    )(*arrays)


SCALE = math.log2(math.e) / math.sqrt(HEAD_DIM)
JOINED = 2
TOGETHER = 2


def stacked(ref, rows, head):
    return jnp.concatenate(
        [ref[rows, (head + j) * HEAD_DIM : (head + j + 1) * HEAD_DIM] for j in range(JOINED)],
        axis=0,
    )


def score_block(query, keys):
    return lax.dot_general(
        query, keys, (((1,), (1,)), ((), ())), preferred_element_type=jnp.float32
    )


def weighted(scores, top, values):
    weights = jnp.concatenate(
        [
            jnp.exp2((scores[:, start : start + HEAD_DIM] - top) * SCALE)
            for start in range(0, scores.shape[1], HEAD_DIM)
        ],
        axis=1,
    )
    both = jnp.concatenate([values, jnp.ones_like(values)], axis=1)
    mixed = jnp.dot(weights.astype(values.dtype), both, preferred_element_type=jnp.float32)
    return mixed[:, :HEAD_DIM], mixed[:, HEAD_DIM:]


def pipelined(tasks, scores_of, rest_of):
    scores = scores_of(*tasks[0])
    for place, task in enumerate(tasks):
        upcoming = scores_of(*tasks[place + 1]) if place + 1 < len(tasks) else None
        rest_of(*task, scores)
        scores = upcoming


def window_kernel(parts, order, flags, query_ref, *rest):
    locals_, (before_ref, after_ref), rest = rest[:parts], rest[parts : parts + 2], rest[parts + 2 :]
    out_ref, level_ref, held = rest
    part, step = pl.program_id(0), pl.program_id(1)
    _, width = query_ref.shape
    grouping = width // HEAD_DIM
    inner = locals_[0].shape[1]
    for r in range(parts):

        @pl.when((part == r) & (step == 0))
        def _(r=r):
            held[:, BLOCK : BLOCK + inner] = locals_[r][...]
            held[:, :BLOCK] = before_ref[...]
            held[:, BLOCK + inner :] = after_ref[...]

    def listed(which, unit):
        place = pl.ds(pl.multiple_of((step * TOGETHER + unit) * BLOCK, BLOCK), WINDOW * BLOCK)
        return held[which, place]

    def scores_of(unit, head):
        block = step * TOGETHER + unit
        scores = score_block(
            stacked(query_ref, slice(unit * BLOCK, (unit + 1) * BLOCK), head), listed(0, unit)
        )
        return jnp.concatenate(
            [
                jnp.where(flags[2 * block] != 0, scores[:, :BLOCK], -1e30),
                scores[:, BLOCK : 2 * BLOCK],
                jnp.where(flags[2 * block + 1] != 0, scores[:, 2 * BLOCK :], -1e30),
            ],
            axis=1,
        )

    def rest_of(unit, head, scores):
        top = jnp.broadcast_to(
            jnp.max(scores, axis=1, keepdims=True), (scores.shape[0], HEAD_DIM)
        )
        mixed, total = weighted(scores, top, listed(1, unit))
        mixed = mixed * (1.0 / total)
        level = top + jnp.log(total) * math.sqrt(HEAD_DIM)
        for j in range(JOINED):
            some = slice(j * BLOCK, (j + 1) * BLOCK)
            rows = slice(unit * BLOCK, (unit + 1) * BLOCK)
            lanes = slice((head + j) * HEAD_DIM, (head + j + 1) * HEAD_DIM)
            out_ref[0, rows, lanes] = mixed[some]
            level_ref[0, rows, lanes] = level[some]

    tasks = [(unit, head) for unit in range(TOGETHER) for head in range(0, grouping, JOINED)]
    pipelined(tasks, scores_of, rest_of)


def whole_block(array):
    return pl.BlockSpec(array.shape, lambda *_: (0,) * array.ndim)


def window_share(order, flags, queries, locals_, edges, begin):
    rows, columns = queries.shape
    heads = edges[0].shape[2] // HEAD_DIM
    width = columns // heads
    blocks = rows // BLOCK
    parts = len(locals_)
    pairs = parts * blocks * (width // HEAD_DIM) * BLOCK * WINDOW * BLOCK
    some = TOGETHER * BLOCK
    edge = pl.BlockSpec((2, BLOCK, HEAD_DIM), lambda r, i, order, flags: (0, 0, order[begin + r]))
    return pl.pallas_call(
        functools.partial(window_kernel, parts),
        grid_spec=pltpu.PrefetchScalarGridSpec(
            num_scalar_prefetch=2,
            grid=(parts, blocks // TOGETHER),
            in_specs=[pl.BlockSpec((some, width), lambda r, i, order, flags: (i, order[begin + r]))]
            + [whole_block(array) for array in locals_]
            + [edge, edge],
            out_specs=[pl.BlockSpec((1, some, width), lambda r, i, order, flags: (r, i, 0))] * 2,
            scratch_shapes=[pltpu.VMEM((2, rows + 2 * BLOCK, HEAD_DIM), queries.dtype)],
        ),
        out_shape=[jax.ShapeDtypeStruct((parts, rows, width), jnp.float32)] * 2,
        compiler_params=pltpu.CompilerParams(vmem_limit_bytes=LESS_VMEM if begin == 0 else MOST_VMEM),
        cost_estimate=pl.CostEstimate(
            flops=4 * pairs * HEAD_DIM, bytes_accessed=8 * MIB, transcendentals=pairs
        ),
        name="window",
    )(order, flags, queries, *locals_, *edges)


LISTED = GLOBALS + RANDOM


def finish_kernel(begin, counts, aliased, order, table, query_ref, mixed_ref, level_ref, *rest):
    sources, (out_ref, held, sems) = rest[: sum(counts)], rest[sum(counts) + aliased :]
    part, step = pl.program_id(0), pl.program_id(1)
    grouping = query_ref.shape[1] // HEAD_DIM
    later, number = [], counts[0]
    for r in range(1, len(counts)):
        start, group = 0, []
        for place, source in enumerate(sources[number : number + counts[r]]):
            rows = source.shape[1]
            group.append(
                pltpu.make_async_copy(
                    source, held.at[r, :, start : start + rows], sems.at[r, place]
                )
            )
            start += rows
        later.append(group)
        number += counts[r]

    @pl.when((part == 0) & (step == 0))
    def _():
        for group in later:
            for copy in group:
                copy.start()
        start = 0
        for source in sources[: counts[0]]:
            held[0, :, start : start + source.shape[1]] = source[...]
            start += source.shape[1]

    for r, group in enumerate(later):

        @pl.when((part == r + 1) & (step == 0))
        def _(group=group):
            for copy in group:
                copy.wait()

    base = ((begin + part) * pl.num_programs(1) + step) * TOGETHER * LISTED

    def listed(which, unit):
        return jnp.concatenate(
            [
                held[
                    part,
                    which,
                    pl.ds(pl.multiple_of(table[base + unit * LISTED + n] * BLOCK, BLOCK), BLOCK),
                ]
                for n in range(LISTED)
            ],
            axis=0,
        )

    def scores_of(unit, head):
        return score_block(
            stacked(query_ref, slice(unit * BLOCK, (unit + 1) * BLOCK), head), listed(0, unit)
        )

    def rest_of(unit, head, scores):
        rows = slice(unit * BLOCK, (unit + 1) * BLOCK)
        level = stacked(level_ref.at[0], rows, head)
        top = jnp.maximum(level, jnp.max(scores, axis=1, keepdims=True))
        mixed, total = weighted(scores, top, listed(1, unit))
        kept = jnp.exp2((level - top) * SCALE)
        inverse = 1.0 / (total + kept)
        mixed = (mixed + stacked(mixed_ref.at[0], rows, head) * kept) * inverse
        for j in range(JOINED):
            lanes = slice((head + j) * HEAD_DIM, (head + j + 1) * HEAD_DIM)
            out_ref[rows, lanes] = mixed[j * BLOCK : (j + 1) * BLOCK].astype(out_ref.dtype)

    tasks = [(unit, head) for unit in range(TOGETHER) for head in range(0, grouping, JOINED)]
    pipelined(tasks, scores_of, rest_of)


def finish(order, table, queries, share, parts, begin, output):
    rows, columns = queries.shape
    width = share[0].shape[2]
    blocks = rows // BLOCK
    arrays = [array for part in parts for array in part]
    pairs = len(parts) * blocks * (width // HEAD_DIM) * BLOCK * LISTED * BLOCK
    some = TOGETHER * BLOCK
    spec = pl.BlockSpec((some, width), lambda r, i, order, table: (i, order[begin + r]))
    aliased = [] if output is None else [output]
    operands = (order, table, queries, *share, *arrays, *aliased)
    return pl.pallas_call(
        functools.partial(finish_kernel, begin, [len(part) for part in parts], len(aliased)),
        grid_spec=pltpu.PrefetchScalarGridSpec(
            num_scalar_prefetch=2,
            grid=(len(parts), blocks // TOGETHER),
            in_specs=[
                spec,
            ]
            + [pl.BlockSpec((1, some, width), lambda r, i, order, table: (r, i, 0))] * 2
            + [whole_block(array) for array in parts[0]]
            + [ANY] * (len(arrays) - len(parts[0]) + len(aliased)),
            out_specs=spec,
            scratch_shapes=[
                pltpu.VMEM(
                    (len(parts), 2, sum(array.shape[1] for array in parts[0]), HEAD_DIM),
                    queries.dtype,
                ),
                pltpu.SemaphoreType.DMA((len(parts), len(parts[0]))),
            ],
        ),
        out_shape=jax.ShapeDtypeStruct((rows, columns), queries.dtype),
        input_output_aliases={len(operands) - 1: 0} if aliased else {},
        compiler_params=pltpu.CompilerParams(vmem_limit_bytes=LESS_VMEM),
        cost_estimate=pl.CostEstimate(
            flops=4 * pairs * HEAD_DIM, bytes_accessed=8 * MIB, transcendentals=pairs
        ),
        name="finish",
    )(*operands)


def plan(random_table, seq_index, head_index, seq_count, heads, my_blocks, slots):
    blocks = random_table.shape[0]
    run_blocks = blocks // seq_count
    by_run = random_table.reshape(seq_count, run_blocks, heads, RANDOM)
    mine = lax.dynamic_index_in_dim(by_run, head_index, 2, keepdims=False)
    mine = mine.reshape(seq_count, run_blocks * RANDOM) - seq_index * run_blocks
    local = jnp.arange(run_blocks, dtype=jnp.int32)
    named = jnp.any(mine[:, None, :] == local[:, None], axis=2)
    rank = jnp.sum(named[:, None, :] & (local[None, :] < local[:, None]), axis=2)
    hit = named[:, None, :] & (rank[:, None, :] == jnp.arange(slots)[:, None])
    sources = jnp.sum(jnp.where(hit, local, 0), axis=2).astype(jnp.int32)
    run = lax.dynamic_index_in_dim(by_run, seq_index, 0, keepdims=False)
    run = run.transpose(1, 0, 2).reshape(heads, run_blocks * RANDOM)
    order_of = jnp.arange(run_blocks * RANDOM)
    earlier = order_of[None, :] < order_of[:, None]
    first = ~jnp.any((run[:, :, None] == run[:, None, :]) & earlier, axis=2)
    start = head_index * my_blocks * RANDOM
    wanted = lax.dynamic_slice_in_dim(run, start, my_blocks * RANDOM, 1)
    same = (wanted[:, :, None] // run_blocks) == (run[:, None, :] // run_blocks)
    below = run[:, None, :] < wanted[:, :, None]
    slot = jnp.sum(same & below & first[:, None, :], axis=2).astype(jnp.int32)
    return sources, wanted // run_blocks, slot


def on_device(query_rows, key_rows, value_rows, random_table, global_blocks):
    seq_count, heads = lax.axis_size("seq"), lax.axis_size("head")
    seq_index, head_index = lax.axis_index("seq"), lax.axis_index("head")
    rows = key_rows.shape[0]
    my_blocks = rows // BLOCK
    run_blocks = my_blocks * heads
    slots = max(1, (RANDOM * run_blocks + 2 * seq_count - 1) // (2 * seq_count))
    order = head_index ^ jnp.arange(heads, dtype=jnp.int32)
    chunk_of = seq_index ^ jnp.arange(seq_count, dtype=jnp.int32)

    def across(array, axis, bit):
        count = lax.axis_size(axis)
        return lax.ppermute(array, axis, [(i, i ^ bit) for i in range(count)])

    *parts, first, last = pack(order, key_rows, value_rows)
    arrived = [parts[0]] + [across(parts[r], "head", r) for r in range(heads - 1, 0, -1)][::-1]

    flat = seq_count * heads
    previous = lax.ppermute(last, ("seq", "head"), [(i, i + 1) for i in range(flat - 1)])
    upcoming = lax.ppermute(first, ("seq", "head"), [(i + 1, i) for i in range(flat - 1)])

    sources, owner, slot = plan(
        random_table, seq_index, head_index, seq_count, heads, my_blocks, slots
    )
    sources = jnp.take(sources, chunk_of, axis=0).reshape(-1)
    shared = jnp.stack(
        [global_blocks % run_blocks, (global_blocks // run_blocks == seq_index).astype(jnp.int32)],
        axis=1,
    ).reshape(-1)
    picked = pick(order, sources, shared, arrived, seq_count, slots)
    outgoing, common = picked[:seq_count], picked[seq_count]
    chunks = [outgoing[0]] + [across(outgoing[k], "seq", k) for k in range(1, seq_count)]
    bit = seq_count // 2
    while bit:
        common = common + across(common, "seq", bit)
        bit //= 2
    half, last_part = seq_count // 2, (seq_count + seq_count // 2) // 2
    own = [join(chunks[:half]), join(chunks[half:last_part]), join(chunks[last_part:] + [common])]
    groups = {0: own}
    bit = heads // 2
    while bit:
        for r in sorted(groups):
            groups[r + bit] = [across(array, "head", bit) for array in groups[r]]
        bit //= 2

    local = jnp.arange(my_blocks, dtype=jnp.int32)
    chunk = owner ^ seq_index
    place = chunk * slots + slot
    place = jnp.take(place, order, axis=0).reshape(heads, my_blocks, RANDOM)
    commons = seq_count * slots + jnp.arange(GLOBALS, dtype=jnp.int32)
    commons = jnp.broadcast_to(commons, (heads, my_blocks, GLOBALS))
    table = jnp.concatenate([commons, place], axis=2).reshape(-1)
    number = (seq_index * heads + head_index) * my_blocks + local
    flags = (
        jnp.stack([number > 0, number < seq_count * run_blocks - 1], axis=1)
        .astype(jnp.int32)
        .reshape(-1)
    )
    half_heads = heads // 2
    shares = []
    for some in (slice(0, half_heads), slice(half_heads, heads)):
        shares.append(
            window_share(order, flags, query_rows, parts[some], (previous, upcoming), some.start)
        )
    output = None
    for n, (begin, end) in enumerate(((0, half_heads), (half_heads, heads))):
        output = finish(
            order,
            table,
            query_rows,
            shares[n],
            [groups[r] for r in range(begin, end)],
            begin,
            output,
        )
    return output


def solution(mesh):
    placed = (
        P(("seq", "head"), None),
        P(("seq", "head"), None),
        P(("seq", "head"), None),
        P(),
        P(),
    )

    return jax.shard_map(
        on_device, mesh=mesh, in_specs=placed, out_specs=P(("seq", "head"), None), check_vma=False
    )
```

```python
import functools
import math

import jax
import jax.numpy as jnp
from jax import lax
from jax.experimental import pallas as pl
from jax.experimental.pallas import tpu as pltpu
from jax.sharding import PartitionSpec as P


BLOCK = 128
HEAD_DIM = 128
GLOBALS = 2
RANDOM = 3
WINDOW = 3
MIB = 2**20
SOME_VMEM = 20 * MIB
MOST_VMEM = 60 * MIB
LESS_VMEM = 50 * MIB


ANY = pl.BlockSpec(memory_space=pl.ANY)
SMEM = pl.BlockSpec(memory_space=pltpu.SMEM)
VMEM = pl.BlockSpec(memory_space=pltpu.VMEM)


def run_copies(copies):
    for copy in copies:
        copy.start()
    for copy in copies:
        copy.wait()


def pack_kernel(heads, order, key_ref, value_ref, *rest):
    outs, first, last = rest[:heads], rest[heads], rest[heads + 1]
    parts, edges, sem_in, sem_out, sem_edge_in, sem_edge_out = rest[heads + 2 :]
    rows = key_ref.shape[0]
    loads = []
    for r in range(heads):
        lanes = pl.ds(pl.multiple_of(order[r] * HEAD_DIM, HEAD_DIM), HEAD_DIM)
        for which, source in enumerate((key_ref, value_ref)):
            loads.append(
                pltpu.make_async_copy(
                    source.at[:, lanes], parts.at[r, which], sem_in.at[r, which]
                )
            )
    for which, source in enumerate((key_ref, value_ref)):
        for side, start in enumerate((0, rows - BLOCK)):
            loads.append(
                pltpu.make_async_copy(
                    source.at[start : start + BLOCK],
                    edges.at[side, which],
                    sem_edge_in.at[side, which],
                )
            )
    run_copies(loads)
    run_copies(
        [pltpu.make_async_copy(parts.at[r], outs[r], sem_out.at[r]) for r in range(heads)]
        + [
            pltpu.make_async_copy(edges.at[side], out, sem_edge_out.at[side])
            for side, out in enumerate((first, last))
        ]
    )


def pack(order, key_rows, value_rows):
    rows, columns = key_rows.shape
    heads = columns // HEAD_DIM
    part = jax.ShapeDtypeStruct((2, rows, HEAD_DIM), key_rows.dtype)
    edge = jax.ShapeDtypeStruct((2, BLOCK, columns), key_rows.dtype)
    return pl.pallas_call(
        functools.partial(pack_kernel, heads),
        in_specs=[SMEM, ANY, ANY],
        out_specs=[ANY] * (heads + 2),
        out_shape=[part] * heads + [edge] * 2,
        scratch_shapes=[
            pltpu.VMEM((heads, 2, rows, HEAD_DIM), key_rows.dtype),
            pltpu.VMEM((2, 2, BLOCK, columns), key_rows.dtype),
            pltpu.SemaphoreType.DMA((heads, 2)),
            pltpu.SemaphoreType.DMA((heads,)),
            pltpu.SemaphoreType.DMA((2, 2)),
            pltpu.SemaphoreType.DMA((2,)),
        ],
        compiler_params=pltpu.CompilerParams(vmem_limit_bytes=SOME_VMEM),
        name="pack",
    )(order, key_rows, value_rows)


def pick_kernel(heads, chunks, slots, order, sources, shared, *rest):
    parts, rest = rest[:heads], rest[heads:]
    outs, shared_ref, (run, sem_in, sem_out) = rest[:chunks], rest[chunks], rest[chunks + 1 :]
    rows = parts[0].shape[1]
    loads = []
    for r in range(heads):
        place = pl.ds(pl.multiple_of(order[r] * rows, BLOCK), rows)
        loads.append(pltpu.make_async_copy(parts[r], run.at[:, place], sem_in.at[r]))
    run_copies(loads)
    stores = []
    for chunk in range(chunks):
        for slot in range(slots):
            place = pl.ds(pl.multiple_of(sources[chunk * slots + slot] * BLOCK, BLOCK), BLOCK)
            stores.append(
                pltpu.make_async_copy(
                    run.at[:, place],
                    outs[chunk].at[:, slot * BLOCK : (slot + 1) * BLOCK],
                    sem_out.at[chunk, slot],
                )
            )
    for copy in stores:
        copy.start()
    for which in range(GLOBALS):
        place = pl.ds(pl.multiple_of(shared[2 * which] * BLOCK, BLOCK), BLOCK)
        block = run[:, place]
        shared_ref[:, which * BLOCK : (which + 1) * BLOCK] = jnp.where(
            shared[2 * which + 1] != 0, block, jnp.zeros_like(block)
        )
    for copy in stores:
        copy.wait()


def pick(order, sources, shared, parts, chunks, slots):
    heads = len(parts)
    rows, dtype = parts[0].shape[1], parts[0].dtype
    return pl.pallas_call(
        functools.partial(pick_kernel, heads, chunks, slots),
        in_specs=[SMEM, SMEM, SMEM] + [ANY] * heads,
        out_specs=[ANY] * chunks + [VMEM],
        out_shape=[jax.ShapeDtypeStruct((2, slots * BLOCK, HEAD_DIM), dtype)] * chunks
        + [jax.ShapeDtypeStruct((2, GLOBALS * BLOCK, HEAD_DIM), dtype)],
        scratch_shapes=[
            pltpu.VMEM((2, heads * rows, HEAD_DIM), dtype),
            pltpu.SemaphoreType.DMA((heads,)),
            pltpu.SemaphoreType.DMA((chunks, slots)),
        ],
        compiler_params=pltpu.CompilerParams(vmem_limit_bytes=SOME_VMEM),
        name="pick",
    )(order, sources, shared, *parts)


def join_kernel(count, *refs):
    sources, out_ref, sems = refs[:count], refs[count], refs[count + 1]
    copies, start = [], 0
    for place, source in enumerate(sources):
        size = source.shape[1]
        copies.append(
            pltpu.make_async_copy(source, out_ref.at[:, start : start + size], sems.at[place])
        )
        start += size
    run_copies(copies)


def join(arrays):
    rows = sum(array.shape[1] for array in arrays)
    shape = (2, rows, HEAD_DIM)
    return pl.pallas_call(
        functools.partial(join_kernel, len(arrays)),
        in_specs=[ANY] * len(arrays),
        out_specs=VMEM,
        out_shape=jax.ShapeDtypeStruct(shape, arrays[0].dtype),
        scratch_shapes=[pltpu.SemaphoreType.DMA((len(arrays),))],
        compiler_params=pltpu.CompilerParams(vmem_limit_bytes=SOME_VMEM),
        name="join",
    )(*arrays)


SCALE = math.log2(math.e) / math.sqrt(HEAD_DIM)
JOINED = 4
TOGETHER = 2


def stacked(ref, rows, head):
    return jnp.concatenate(
        [ref[rows, (head + j) * HEAD_DIM : (head + j + 1) * HEAD_DIM] for j in range(JOINED)],
        axis=0,
    )


def score_block(query, keys):
    return lax.dot_general(
        query, keys, (((1,), (1,)), ((), ())), preferred_element_type=jnp.float32
    )


def weighted(scores, top, values):
    weights = jnp.concatenate(
        [
            jnp.exp2((scores[:, start : start + HEAD_DIM] - top) * SCALE)
            for start in range(0, scores.shape[1], HEAD_DIM)
        ],
        axis=1,
    )
    both = jnp.concatenate([values, jnp.ones_like(values)], axis=1)
    mixed = jnp.dot(weights.astype(values.dtype), both, preferred_element_type=jnp.float32)
    return mixed[:, :HEAD_DIM], mixed[:, HEAD_DIM:]


def pipelined(tasks, scores_of, rest_of):
    scores = scores_of(*tasks[0])
    for place, task in enumerate(tasks):
        upcoming = scores_of(*tasks[place + 1]) if place + 1 < len(tasks) else None
        rest_of(*task, scores)
        scores = upcoming


def window_kernel(parts, order, flags, query_ref, *rest):
    locals_, (before_ref, after_ref), rest = rest[:parts], rest[parts : parts + 2], rest[parts + 2 :]
    out_ref, level_ref, held = rest
    part, step = pl.program_id(0), pl.program_id(1)
    _, width = query_ref.shape
    grouping = width // HEAD_DIM
    inner = locals_[0].shape[1]
    for r in range(parts):

        @pl.when((part == r) & (step == 0))
        def _(r=r):
            held[:, BLOCK : BLOCK + inner] = locals_[r][...]
            held[:, :BLOCK] = before_ref[...]
            held[:, BLOCK + inner :] = after_ref[...]

    def listed(which, unit):
        place = pl.ds(pl.multiple_of((step * TOGETHER + unit) * BLOCK, BLOCK), WINDOW * BLOCK)
        return held[which, place]

    def scores_of(unit, head):
        block = step * TOGETHER + unit
        scores = score_block(
            stacked(query_ref, slice(unit * BLOCK, (unit + 1) * BLOCK), head), listed(0, unit)
        )
        return jnp.concatenate(
            [
                jnp.where(flags[2 * block] != 0, scores[:, :BLOCK], -1e30),
                scores[:, BLOCK : 2 * BLOCK],
                jnp.where(flags[2 * block + 1] != 0, scores[:, 2 * BLOCK :], -1e30),
            ],
            axis=1,
        )

    def rest_of(unit, head, scores):
        top = jnp.broadcast_to(
            jnp.max(scores, axis=1, keepdims=True), (scores.shape[0], HEAD_DIM)
        )
        mixed, total = weighted(scores, top, listed(1, unit))
        mixed = mixed * (1.0 / total)
        level = top + jnp.log(total) * math.sqrt(HEAD_DIM)
        for j in range(JOINED):
            some = slice(j * BLOCK, (j + 1) * BLOCK)
            rows = slice(unit * BLOCK, (unit + 1) * BLOCK)
            lanes = slice((head + j) * HEAD_DIM, (head + j + 1) * HEAD_DIM)
            out_ref[0, rows, lanes] = mixed[some]
            level_ref[0, rows, lanes] = level[some]

    tasks = [(unit, head) for unit in range(TOGETHER) for head in range(0, grouping, JOINED)]
    pipelined(tasks, scores_of, rest_of)


def whole_block(array):
    return pl.BlockSpec(array.shape, lambda *_: (0,) * array.ndim)


def window_share(order, flags, queries, locals_, edges, begin):
    rows, columns = queries.shape
    heads = edges[0].shape[2] // HEAD_DIM
    width = columns // heads
    blocks = rows // BLOCK
    parts = len(locals_)
    pairs = parts * blocks * (width // HEAD_DIM) * BLOCK * WINDOW * BLOCK
    some = TOGETHER * BLOCK
    edge = pl.BlockSpec((2, BLOCK, HEAD_DIM), lambda r, i, order, flags: (0, 0, order[begin + r]))
    return pl.pallas_call(
        functools.partial(window_kernel, parts),
        grid_spec=pltpu.PrefetchScalarGridSpec(
            num_scalar_prefetch=2,
            grid=(parts, blocks // TOGETHER),
            in_specs=[pl.BlockSpec((some, width), lambda r, i, order, flags: (i, order[begin + r]))]
            + [whole_block(array) for array in locals_]
            + [edge, edge],
            out_specs=[pl.BlockSpec((1, some, width), lambda r, i, order, flags: (r, i, 0))] * 2,
            scratch_shapes=[pltpu.VMEM((2, rows + 2 * BLOCK, HEAD_DIM), queries.dtype)],
        ),
        out_shape=[jax.ShapeDtypeStruct((parts, rows, width), jnp.float32)] * 2,
        compiler_params=pltpu.CompilerParams(vmem_limit_bytes=LESS_VMEM if begin == 0 else MOST_VMEM),
        cost_estimate=pl.CostEstimate(
            flops=4 * pairs * HEAD_DIM, bytes_accessed=8 * MIB, transcendentals=pairs
        ),
        name="window",
    )(order, flags, queries, *locals_, *edges)


LISTED = GLOBALS + RANDOM


def finish_kernel(begin, counts, aliased, order, table, query_ref, mixed_ref, level_ref, *rest):
    sources, (out_ref, held, sems) = rest[: sum(counts)], rest[sum(counts) + aliased :]
    part, step = pl.program_id(0), pl.program_id(1)
    grouping = query_ref.shape[1] // HEAD_DIM
    later, number = [], counts[0]
    for r in range(1, len(counts)):
        start, group = 0, []
        for place, source in enumerate(sources[number : number + counts[r]]):
            rows = source.shape[1]
            group.append(
                pltpu.make_async_copy(
                    source, held.at[r, :, start : start + rows], sems.at[r, place]
                )
            )
            start += rows
        later.append(group)
        number += counts[r]

    @pl.when((part == 0) & (step == 0))
    def _():
        for group in later:
            for copy in group:
                copy.start()
        start = 0
        for source in sources[: counts[0]]:
            held[0, :, start : start + source.shape[1]] = source[...]
            start += source.shape[1]

    for r, group in enumerate(later):

        @pl.when((part == r + 1) & (step == 0))
        def _(group=group):
            for copy in group:
                copy.wait()

    base = ((begin + part) * pl.num_programs(1) + step) * TOGETHER * LISTED

    def listed(which, unit):
        return jnp.concatenate(
            [
                held[
                    part,
                    which,
                    pl.ds(pl.multiple_of(table[base + unit * LISTED + n] * BLOCK, BLOCK), BLOCK),
                ]
                for n in range(LISTED)
            ],
            axis=0,
        )

    def scores_of(unit, head):
        return score_block(
            stacked(query_ref, slice(unit * BLOCK, (unit + 1) * BLOCK), head), listed(0, unit)
        )

    def rest_of(unit, head, scores):
        rows = slice(unit * BLOCK, (unit + 1) * BLOCK)
        level = stacked(level_ref.at[0], rows, head)
        top = jnp.maximum(level, jnp.max(scores, axis=1, keepdims=True))
        mixed, total = weighted(scores, top, listed(1, unit))
        kept = jnp.exp2((level - top) * SCALE)
        inverse = 1.0 / (total + kept)
        mixed = (mixed + stacked(mixed_ref.at[0], rows, head) * kept) * inverse
        for j in range(JOINED):
            lanes = slice((head + j) * HEAD_DIM, (head + j + 1) * HEAD_DIM)
            out_ref[rows, lanes] = mixed[j * BLOCK : (j + 1) * BLOCK].astype(out_ref.dtype)

    tasks = [(unit, head) for unit in range(TOGETHER) for head in range(0, grouping, JOINED)]
    pipelined(tasks, scores_of, rest_of)


def finish(order, table, queries, share, parts, begin, output):
    rows, columns = queries.shape
    width = share[0].shape[2]
    blocks = rows // BLOCK
    arrays = [array for part in parts for array in part]
    pairs = len(parts) * blocks * (width // HEAD_DIM) * BLOCK * LISTED * BLOCK
    some = TOGETHER * BLOCK
    spec = pl.BlockSpec((some, width), lambda r, i, order, table: (i, order[begin + r]))
    aliased = [] if output is None else [output]
    operands = (order, table, queries, *share, *arrays, *aliased)
    return pl.pallas_call(
        functools.partial(finish_kernel, begin, [len(part) for part in parts], len(aliased)),
        grid_spec=pltpu.PrefetchScalarGridSpec(
            num_scalar_prefetch=2,
            grid=(len(parts), blocks // TOGETHER),
            in_specs=[
                spec,
            ]
            + [pl.BlockSpec((1, some, width), lambda r, i, order, table: (r, i, 0))] * 2
            + [whole_block(array) for array in parts[0]]
            + [ANY] * (len(arrays) - len(parts[0]) + len(aliased)),
            out_specs=spec,
            scratch_shapes=[
                pltpu.VMEM(
                    (len(parts), 2, sum(array.shape[1] for array in parts[0]), HEAD_DIM),
                    queries.dtype,
                ),
                pltpu.SemaphoreType.DMA((len(parts), len(parts[0]))),
            ],
        ),
        out_shape=jax.ShapeDtypeStruct((rows, columns), queries.dtype),
        input_output_aliases={len(operands) - 1: 0} if aliased else {},
        compiler_params=pltpu.CompilerParams(vmem_limit_bytes=LESS_VMEM),
        cost_estimate=pl.CostEstimate(
            flops=4 * pairs * HEAD_DIM, bytes_accessed=8 * MIB, transcendentals=pairs
        ),
        name="finish",
    )(*operands)


def plan(random_table, seq_index, head_index, seq_count, heads, my_blocks, slots):
    blocks = random_table.shape[0]
    run_blocks = blocks // seq_count
    by_run = random_table.reshape(seq_count, run_blocks, heads, RANDOM)
    mine = lax.dynamic_index_in_dim(by_run, head_index, 2, keepdims=False)
    mine = mine.reshape(seq_count, run_blocks * RANDOM) - seq_index * run_blocks
    local = jnp.arange(run_blocks, dtype=jnp.int32)
    named = jnp.any(mine[:, None, :] == local[:, None], axis=2)
    rank = jnp.sum(named[:, None, :] & (local[None, :] < local[:, None]), axis=2)
    hit = named[:, None, :] & (rank[:, None, :] == jnp.arange(slots)[:, None])
    sources = jnp.sum(jnp.where(hit, local, 0), axis=2).astype(jnp.int32)
    run = lax.dynamic_index_in_dim(by_run, seq_index, 0, keepdims=False)
    run = run.transpose(1, 0, 2).reshape(heads, run_blocks * RANDOM)
    order_of = jnp.arange(run_blocks * RANDOM)
    earlier = order_of[None, :] < order_of[:, None]
    first = ~jnp.any((run[:, :, None] == run[:, None, :]) & earlier, axis=2)
    start = head_index * my_blocks * RANDOM
    wanted = lax.dynamic_slice_in_dim(run, start, my_blocks * RANDOM, 1)
    same = (wanted[:, :, None] // run_blocks) == (run[:, None, :] // run_blocks)
    below = run[:, None, :] < wanted[:, :, None]
    slot = jnp.sum(same & below & first[:, None, :], axis=2).astype(jnp.int32)
    return sources, wanted // run_blocks, slot


def on_device(query_rows, key_rows, value_rows, random_table, global_blocks):
    seq_count, heads = lax.axis_size("seq"), lax.axis_size("head")
    seq_index, head_index = lax.axis_index("seq"), lax.axis_index("head")
    rows = key_rows.shape[0]
    my_blocks = rows // BLOCK
    run_blocks = my_blocks * heads
    slots = max(1, (RANDOM * run_blocks + 2 * seq_count - 1) // (2 * seq_count))
    order = head_index ^ jnp.arange(heads, dtype=jnp.int32)
    chunk_of = seq_index ^ jnp.arange(seq_count, dtype=jnp.int32)

    def across(array, axis, bit):
        count = lax.axis_size(axis)
        return lax.ppermute(array, axis, [(i, i ^ bit) for i in range(count)])

    *parts, first, last = pack(order, key_rows, value_rows)
    arrived = [parts[0]] + [across(parts[r], "head", r) for r in range(heads - 1, 0, -1)][::-1]

    flat = seq_count * heads
    previous = lax.ppermute(last, ("seq", "head"), [(i, i + 1) for i in range(flat - 1)])
    upcoming = lax.ppermute(first, ("seq", "head"), [(i + 1, i) for i in range(flat - 1)])

    sources, owner, slot = plan(
        random_table, seq_index, head_index, seq_count, heads, my_blocks, slots
    )
    sources = jnp.take(sources, chunk_of, axis=0).reshape(-1)
    shared = jnp.stack(
        [global_blocks % run_blocks, (global_blocks // run_blocks == seq_index).astype(jnp.int32)],
        axis=1,
    ).reshape(-1)
    picked = pick(order, sources, shared, arrived, seq_count, slots)
    outgoing, common = picked[:seq_count], picked[seq_count]
    chunks = [outgoing[0]] + [across(outgoing[k], "seq", k) for k in range(1, seq_count)]
    bit = seq_count // 2
    while bit:
        common = common + across(common, "seq", bit)
        bit //= 2
    half, last_part = seq_count // 2, (seq_count + seq_count // 2) // 2
    own = [
        chunks[0],
        join(chunks[1:half]),
        join(chunks[half:last_part]),
        join(chunks[last_part:] + [common]),
    ]
    groups = {0: own}
    bit = heads // 2
    while bit:
        for r in sorted(groups):
            groups[r + bit] = [across(array, "head", bit) for array in groups[r]]
        bit //= 2

    local = jnp.arange(my_blocks, dtype=jnp.int32)
    chunk = owner ^ seq_index
    place = chunk * slots + slot
    place = jnp.take(place, order, axis=0).reshape(heads, my_blocks, RANDOM)
    commons = seq_count * slots + jnp.arange(GLOBALS, dtype=jnp.int32)
    commons = jnp.broadcast_to(commons, (heads, my_blocks, GLOBALS))
    table = jnp.concatenate([commons, place], axis=2).reshape(-1)
    number = (seq_index * heads + head_index) * my_blocks + local
    flags = (
        jnp.stack([number > 0, number < seq_count * run_blocks - 1], axis=1)
        .astype(jnp.int32)
        .reshape(-1)
    )
    half_heads = heads // 2
    shares = []
    for some in (slice(0, half_heads), slice(half_heads, heads)):
        shares.append(
            window_share(order, flags, query_rows, parts[some], (previous, upcoming), some.start)
        )
    output = None
    for n, (begin, end) in enumerate(((0, half_heads), (half_heads, heads))):
        output = finish(
            order,
            table,
            query_rows,
            shares[n],
            [groups[r] for r in range(begin, end)],
            begin,
            output,
        )
    return output


def solution(mesh):
    placed = (
        P(("seq", "head"), None),
        P(("seq", "head"), None),
        P(("seq", "head"), None),
        P(),
        P(),
    )

    return jax.shard_map(
        on_device, mesh=mesh, in_specs=placed, out_specs=P(("seq", "head"), None), check_vma=False
    )
```
